128 devices in a mesh: col: 16 (over y, z), row: 8 (over x, core).
Axes of the slice: x: 4, y: 4, z: 4, core: 2. Of those that a mesh axis runs over, the one named last changes fastest.
Arguments:
- u_factors: bfloat16 [2, 64, 256, 64, 128], P(None, 'row', None, 'col'), may hold values from -0.09375 to 0.09375
- v_factors: bfloat16 [2, 64, 256, 64, 128], P(None, 'row', None, 'col'), may hold values from -0.375 to 0.375
- ranks: int32 [2, 64, 64], P(None, 'row', 'col'), may hold values from 8 to 64
- model_init: float32 [2, 16384, 256], P(None, ('col', 'row')), may hold values from -6 to 6
- observed: float32 [2, 16384, 256], P(None, ('row', 'col')), may hold values from -6 to 6
- step: float32 [2], replicated, may hold values from 0.1 to 0.4
Outputs:
- model: float32 [2, 16384, 256], P(None, ('col', 'row'))
- misfit: float32 [2, 16384, 256], P(None, ('row', 'col'))
The draws below stay inside these ranges and needn't reach their ends.
Inputs may be any that keep to these rules, and one draw needn't show every extreme that they name: `ranks`: columns of a factor beyond its tile's rank do not count.
All inputs are finite; a program needn't handle non-finite values.
Results may differ from the reference program's by a relative error of at most 0.0085.
Values may be sent and summed in bfloat16 or wider, within the bound.
A program may use at most 128 MiB of HBM per device.

```python
import math
import jax
import jax.numpy as jnp
from jax import lax

ORDER = 16384
TILE = 256
RMAX = 64
RHS = 128
FREQS = 2
ITERS = 2
TILES = 64


def touch_ends(drawn, rng, least, high):
    longest = drawn.shape.index(max(drawn.shape))
    spots = []
    for shift in (0, 1):
        where = [jax.random.randint(jax.random.fold_in(rng, axis), (), 0, length) for axis, length in enumerate(drawn.shape)]
        where[longest] = (where[longest] + shift) % drawn.shape[longest]
        spots.append(tuple(where))
    return drawn.at[spots[0]].set(least).at[spots[1]].set(high)


def block_levels(own_key, dims, cuts, smallest, high):
    loudness, own = 1.0, jax.random.fold_in(own_key, 6)
    for axis_at, blocks in cuts:
        steps = jnp.exp(jax.random.uniform(jax.random.fold_in(own, axis_at), (blocks,), jnp.float32, smallest / len(cuts), high / len(cuts)))
        loudness = loudness * jnp.repeat(steps, dims[axis_at] // blocks).reshape([-1 if axis == axis_at else 1 for axis in range(len(dims))])
    return loudness


def noise(rng, shape, scale, reach, cuts=(), kind=jnp.bfloat16):
    result = jax.random.normal(rng, shape, jnp.float32) * scale
    if len(cuts) > 0:
        result = block_levels(rng, shape, cuts, -0.22, 0.18) * result
    return jnp.clip(result, min=-reach, max=reach).astype(kind)


def setup_inputs(seed: int = 0) -> dict:
    arg_keys = jax.random.split(jax.random.key(seed), 7)
    u_factors = noise(arg_keys[0], (FREQS, TILES, TILE, TILES, 2 * RMAX), (TILES * RMAX) ** -0.5, 0.09375, ((1, 8), (3, 16)))
    v_factors = noise(arg_keys[1], (FREQS, TILES, TILE, TILES, 2 * RMAX), TILE ** -0.5, 0.375, ((1, 8), (3, 16)))
    ranks = touch_ends(jax.random.randint(arg_keys[2], (FREQS, TILES, TILES), RMAX // 8, RMAX + 1), jax.random.fold_in(arg_keys[2], 1), RMAX // 8, RMAX).astype(jnp.int32)
    model_init = noise(arg_keys[3], (FREQS, ORDER, 2 * RHS), 1.0, 6.0, ((1, 128),), jnp.float32)
    observed = noise(arg_keys[4], (FREQS, ORDER, 2 * RHS), 1.0, 6.0, ((1, 128),), jnp.float32)
    step = jnp.clip(jnp.exp(jax.random.uniform(arg_keys[5], (FREQS,), jnp.float32, math.log(0.1), math.log(0.4))), 0.1, 0.4)
    return dict(u_factors=u_factors, v_factors=v_factors, ranks=ranks, model_init=model_init, observed=observed, step=step)


def split_product(product, rank_mask):
    real = product[..., :RMAX, :RHS] + product[..., RMAX:, RHS:]
    imaginary = product[..., :RMAX, RHS:] - product[..., RMAX:, :RHS]
    weights = rank_mask[..., None]
    return jnp.concatenate([real * weights, imaginary * weights], -1).astype(jnp.bfloat16)


def expand_complex(coefficient):
    real = coefficient[..., :RHS]
    imaginary = coefficient[..., RHS:]
    upper = jnp.concatenate([real, imaginary], -1)
    lower = jnp.concatenate([-imaginary, real], -1)
    return jnp.concatenate([upper, lower], -2).astype(jnp.float32)


def reference(u_factors, v_factors, ranks, model_init, observed, step):
    rank_mask = (jnp.arange(RMAX, dtype=jnp.int32)[None, None, None, :] < ranks[..., None]).astype(jnp.float32)
    model = model_init
    misfit = model_init
    for sweep in range(ITERS):
        model_half = model.astype(jnp.bfloat16).astype(jnp.float32).reshape(FREQS, TILES, TILE, 2 * RHS)

        def forward_row(tile_row):
            left = u_factors[:, tile_row].astype(jnp.float32)
            right = v_factors[:, tile_row].astype(jnp.float32)
            product = jnp.einsum('fajk,fjal->fjkl', right, model_half)
            coefficient = split_product(product, rank_mask[:, tile_row])
            return jnp.einsum('fajk,fjkl->fal', left, expand_complex(coefficient))

        predicted = lax.map(forward_row, jnp.arange(TILES, dtype=jnp.int32))
        predicted = predicted.transpose(1, 0, 2, 3).reshape(FREQS, ORDER, 2 * RHS)
        misfit = predicted - observed
        misfit_half = misfit.astype(jnp.bfloat16).astype(jnp.float32).reshape(FREQS, TILES, TILE, 2 * RHS)

        def adjoint_row(running, tile_row):
            left = u_factors[:, tile_row].astype(jnp.float32)
            right = v_factors[:, tile_row].astype(jnp.float32)
            rows_here = lax.dynamic_index_in_dim(misfit_half, tile_row, 1, keepdims=False)
            product = jnp.einsum('fajk,fal->fjkl', left, rows_here)
            back = split_product(product, rank_mask[:, tile_row])
            return running + jnp.einsum('fajk,fjkl->fjal', right, expand_complex(back)), None

        start = jnp.zeros((FREQS, TILES, TILE, 2 * RHS), jnp.float32)
        gradient, unused = lax.scan(adjoint_row, start, jnp.arange(TILES, dtype=jnp.int32))
        model = model - step[:, None, None] * gradient.reshape(FREQS, ORDER, 2 * RHS)
    return model, misfit
```

```python
import jax
import jax.numpy as jnp
from jax import lax
from jax.sharding import PartitionSpec as P

ITERS = 2


def split_product(product, rank_mask, rank_most, right_count):
    real = product[..., :rank_most, :right_count] + product[..., rank_most:, right_count:]
    imaginary = product[..., :rank_most, right_count:] - product[..., rank_most:, :right_count]
    weights = rank_mask[..., None]
    return jnp.concatenate([real * weights, imaginary * weights], -1).astype(jnp.bfloat16)


def expand_complex(coefficient, right_count):
    real = coefficient[..., :right_count]
    imaginary = coefficient[..., right_count:]
    upper = jnp.concatenate([real, imaginary], -1)
    lower = jnp.concatenate([-imaginary, real], -1)
    return jnp.concatenate([upper, lower], -2)


def local(u_factors, v_factors, ranks, model_init, observed, step):
    frequencies = model_init.shape[0]
    rank_most = u_factors.shape[-1] // 2
    right_count = model_init.shape[-1] // 2
    tile_size = u_factors.shape[2]
    rows_here = u_factors.shape[1]
    cols_here = u_factors.shape[3]
    rank_mask = (
        jnp.arange(rank_most, dtype=jnp.int32)[None, None, None, :] < ranks[..., None]
    ).astype(jnp.float32)
    model = model_init
    misfit = model_init
    for sweep in range(ITERS):
        gathered = lax.all_gather(model.astype(jnp.bfloat16), "row", axis=1, tiled=True)
        model_tiles = gathered.reshape(frequencies, cols_here, tile_size, 2 * right_count)
        product = jnp.einsum(
            "fiajk,fjal->fijkl", v_factors, model_tiles, preferred_element_type=jnp.float32
        )
        coefficient = expand_complex(
            split_product(product, rank_mask, rank_most, right_count), right_count
        )
        partial_value = jnp.einsum(
            "fiajk,fijkl->fial", u_factors, coefficient, preferred_element_type=jnp.float32
        )
        partial_value = partial_value.reshape(frequencies, rows_here * tile_size, 2 * right_count)
        predicted = lax.psum_scatter(
            partial_value.astype(jnp.bfloat16), "col", scatter_dimension=1, tiled=True
        )
        misfit = predicted.astype(jnp.float32) - observed
        misfit_half = lax.all_gather(
            misfit.astype(jnp.bfloat16), "col", axis=1, tiled=True
        )
        misfit_tiles = misfit_half.reshape(frequencies, rows_here, tile_size, 2 * right_count)
        product = jnp.einsum(
            "fiajk,fial->fijkl", u_factors, misfit_tiles, preferred_element_type=jnp.float32
        )
        back = expand_complex(
            split_product(product, rank_mask, rank_most, right_count), right_count
        )
        gradient_part = jnp.einsum(
            "fiajk,fijkl->fjal", v_factors, back, preferred_element_type=jnp.float32
        )
        gradient_part = gradient_part.reshape(frequencies, cols_here * tile_size, 2 * right_count)
        gradient = lax.psum_scatter(
            gradient_part.astype(jnp.bfloat16), "row", scatter_dimension=1, tiled=True
        ).astype(jnp.float32)
        model = model - step[:, None, None] * gradient
    return (model, misfit)


def solution(mesh):
    return jax.shard_map(
        local,
        mesh=mesh,
        in_specs=(
            P(None, "row", None, "col", None),
            P(None, "row", None, "col", None),
            P(None, "row", "col"),
            P(None, ("col", "row"), None),
            P(None, ("row", "col"), None),
            P(),
        ),
        out_specs=(P(None, ("col", "row"), None), P(None, ("row", "col"), None)),
        check_vma=False,
    )
```

```python
import functools

import jax
import jax.numpy as jnp
from jax import lax
from jax.experimental import pallas as pl
from jax.experimental.pallas import tpu as pltpu
from jax.sharding import PartitionSpec as P

ITERS = 2
MESH = pl.DeviceIdType.MESH
F32, BF16 = jnp.float32, jnp.bfloat16
LANES = 128
TRANS_B = (((1,), (1,)), ((), ()))


def kernel(
    u_hbm, v_hbm, ranks, model_in, observed, step,
    model_out, misfit_out,
    u_raw, v_raw, u_tiles, v_tiles, wide, expanded_f, expanded_b,
    model_t, observed_t, misfit_t,
    x_all, sum_a, sum_b, got_a, got_b, keep_a, keep_b, next_a, next_b, last_a, last_b,
    r_a, r_b, grad, grad_got, grad_keep, grad_send, grad_last,
    load_sem, send_sem, recv_sem,
):
    freqs, rows, cols = u_raw.shape[0], u_raw.shape[1], v_tiles.shape[1]
    tile = v_tiles.shape[2]
    half = tile // 2
    col, row = lax.axis_index("col"), lax.axis_index("row")
    y, z = col // 4, col % 4
    x, core = row // 2, row % 2

    def at_y(o):
        return ((y + o) % 4 * 4 + z, row)

    def at_z(o):
        return (y * 4 + (z + o) % 4, row)

    def at_x(o):
        return (col, (x + o) % 4 * 2 + core)

    partner = (col, x * 2 + 1 - core)
    numbers = {}

    def remote(name, src, dst, device):
        number = numbers.setdefault(name, len(numbers))
        return pltpu.make_async_remote_copy(
            src_ref=src, dst_ref=dst, send_sem=send_sem.at[number], recv_sem=recv_sem.at[number],
            device_id=device, device_id_type=MESH,
        )

    loads = {}
    for f in range(freqs):
        for n, (src, dst) in enumerate(((v_hbm, v_raw), (u_hbm, u_raw))):
            loads[f, n] = pltpu.make_async_copy(src.at[f], dst.at[f], load_sem.at[2 * f + n])
            loads[f, n].start()

    barrier = pltpu.get_barrier_semaphore()
    peers = [at_y(o) for o in (1, 2, 3)] + [at_z(o) for o in (1, 2, 3)] + [at_x(o) for o in (1, 2, 3)] + [partner]
    for peer in peers:
        pl.semaphore_signal(barrier, inc=1, device_id=peer, device_id_type=MESH)

    for f in range(freqs):
        turned = model_in[f].T
        model_t[f] = turned
        x_all[f, row] = turned.astype(BF16)
    pl.semaphore_wait(barrier, len(peers))

    lane = lax.broadcasted_iota(jnp.int32, (1, LANES), 1)
    sign = jnp.where(lane < LANES // 2, 1.0, -1.0).astype(F32)
    lane_k = lane % (LANES // 2)

    def relayout(f, raw, put):
        def one(i, carry):
            wide[...] = raw[f, i].astype(F32)
            for j in range(cols):
                piece = wide[pl.ds(j, tile, stride=cols), :]
                piece = jnp.where(lane_k < ranks[(f * rows + i) * cols + j], piece, 0.0)
                put(i, j, piece.astype(BF16))
            return carry

        lax.fori_loop(0, rows, one, 0)

    def relayout_v(f):
        loads[f, 0].wait()

        def put(i, j, piece):
            v_tiles[f, j, :, pl.ds(pl.multiple_of(i * LANES, LANES), LANES)] = piece

        relayout(f, v_raw, put)

    def relayout_u(f):
        loads[f, 1].wait()

        def put(i, j, piece):
            u_tiles[f, i, :, j * LANES:(j + 1) * LANES] = piece

        relayout(f, u_raw, put)

    def gather_x_copies(f):
        own = x_all.at[f, row]
        return [remote(("a", f, o), own, own, at_x(o)) for o in (1, 3, 2)] + [remote(("a", f, 0), own, own, partner)]

    def gather_x_pass(f):
        copies = []
        for o in (1, 3, 2):
            slot = x_all.at[f, (x - o + 4) % 4 * 2 + core]
            copies.append(remote(("ap", f, o), slot, slot, partner))
        return copies

    def gather_x_start(f):
        for copy in gather_x_copies(f):
            copy.start()

    def gather_x_mid(f):
        for copy, onward in zip(gather_x_copies(f)[:3], gather_x_pass(f)):
            copy.wait_recv()
            onward.start()

    def gather_x_end(f):
        copies = gather_x_copies(f)
        copies[3].wait_recv()
        for onward in gather_x_pass(f):
            onward.wait()
        for copy in copies:
            copy.wait_send()

    def expand(top, bottom):
        return (
            (top + sign * pltpu.roll(bottom, LANES // 2, 1)).astype(BF16),
            (bottom - sign * pltpu.roll(top, LANES // 2, 1)).astype(BF16),
        )

    def forward_products(f):
        def one(j, carry):
            left = jnp.concatenate([x_all[f, 2 * j], x_all[f, 2 * j + 1]], axis=1)
            product = jnp.dot(left, v_tiles[f, j], preferred_element_type=F32)
            for i in range(rows):
                part = product[:, i * LANES:(i + 1) * LANES]
                top, bottom = expand(part[:half], part[half:])
                at = pl.ds(pl.multiple_of(j * LANES, LANES), LANES)
                expanded_f[i, :half, at] = top
                expanded_f[i, half:, at] = bottom
            return carry

        lax.fori_loop(0, cols, one, 0)

    def forward_sums(f):
        def one(i, carry):
            total = lax.dot_general(expanded_f[i], u_tiles[f, i], TRANS_B, preferred_element_type=F32)
            total = total.astype(BF16)
            for h in range(2):
                part = total[:, h * LANES:(h + 1) * LANES]
                sum_a[f, 2 * i + h] = part[:half]
                sum_b[f, (2 * (i % 2) + h) * 4 + i // 2] = part[half:]
            return carry

        lax.fori_loop(0, rows, one, 0)

    def first_copies(f):
        copies = []
        for o in (2, 1, 3):
            copies.append(remote(("c1a", f, o), sum_a.at[f, pl.ds((y + o) % 4 * 4, 4)], got_a.at[f, o - 1], at_y(o)))
            copies.append(remote(("c1b", f, o), sum_b.at[f, pl.ds((z + o) % 4 * 4, 4)], got_b.at[f, o - 1], at_z(o)))
        return copies

    def second_copies(f):
        copies = []
        for o in (2, 1, 3):
            copies.append(remote(("c2a", f, o), next_a.at[f, (z + o) % 4], last_a.at[f, o - 1], at_z(o)))
            copies.append(remote(("c2b", f, o), next_b.at[f, (y + o) % 4], last_b.at[f, o - 1], at_y(o)))
        return copies

    def start(copies):
        for copy in copies:
            copy.start()

    def wait(copies):
        for copy in copies:
            copy.wait()

    def first_end(f):
        wait(first_copies(f))
        for q in range(4):
            for own, got, keep, onward, at in (
                (sum_a, got_a, keep_a, next_a, y), (sum_b, got_b, keep_b, next_b, z)
            ):
                total = own[f, at * 4 + q].astype(F32)
                for o in range(3):
                    total = total + got[f, o, q].astype(F32)
                keep[f, q] = total
                onward[f, q] = total.astype(BF16)
        start(second_copies(f))

    def gather_first(f):
        copies = []
        own_a, own_b = r_a.at[f, y * 4 + z], r_b.at[f, z * 4 + y]
        for o in (2, 1, 3):
            copies.append(remote(("e1a", f, o), own_a, own_a, at_z(o)))
            copies.append(remote(("e1b", f, o), own_b, own_b, at_y(o)))
        return copies

    def gather_second(f):
        copies = []
        own_a, own_b = r_a.at[f, pl.ds(y * 4, 4)], r_b.at[f, pl.ds(z * 4, 4)]
        for o in (2, 1, 3):
            copies.append(remote(("e2a", f, o), own_a, own_a, at_y(o)))
            copies.append(remote(("e2b", f, o), own_b, own_b, at_z(o)))
        return copies

    def second_end(f, last):
        wait(second_copies(f))
        for keep, got, to, rows_at, at, slot in (
            (keep_a, last_a, r_a, slice(0, half), z, y * 4 + z),
            (keep_b, last_b, r_b, slice(half, tile), y, z * 4 + y),
        ):
            total = keep[f, at]
            for o in range(3):
                total = total + got[f, o].astype(F32)
            total = total - observed_t[f, rows_at]
            if last:
                misfit_t[f, rows_at] = total
            to[f, slot] = total.astype(BF16)
        start(gather_first(f))

    def backward_products(f):
        def one(i, carry):
            left_a = jnp.concatenate([r_a[f, 2 * i], r_a[f, 2 * i + 1]], axis=1)
            at_b = 2 * (i % 2) * 4 + i // 2
            left_b = jnp.concatenate([r_b[f, at_b], r_b[f, at_b + 4]], axis=1)
            left = jnp.concatenate([left_a, left_b], axis=0)
            product = jnp.dot(left, u_tiles[f, i], preferred_element_type=F32)
            for j in range(cols):
                part = product[:, j * LANES:(j + 1) * LANES]
                top, bottom = expand(part[:half], part[half:])
                at = pl.ds(pl.multiple_of(i * LANES, LANES), LANES)
                expanded_b[j, :half, at] = top
                expanded_b[j, half:, at] = bottom
            return carry

        lax.fori_loop(0, rows, one, 0)

    def pair_copy(f, j):
        return remote(("g1", f, j), grad.at[f, 1 - core, j], grad_got.at[f, j], partner)

    def backward_sums(f):
        for j in range(cols):
            total = lax.dot_general(expanded_b[j], v_tiles[f, j], TRANS_B, preferred_element_type=F32)
            for h in range(2):
                grad[f, h, j] = total[:, h * LANES:(h + 1) * LANES]
            pair_copy(f, j).start()

    def across_copies(f):
        return [
            remote(("g2", f, o), grad_send.at[f, (x + o) % 4], grad_last.at[f, o - 1], at_x(o)) for o in (2, 1, 3)
        ]

    def pair_end(f):
        for j in range(cols):
            pair_copy(f, j).wait()
            total = grad[f, core, j] + grad_got[f, j]
            grad_keep[f, j] = total
            grad_send[f, j] = total.astype(BF16)
        start(across_copies(f))

    def across_end(f, last):
        wait(across_copies(f))
        total = grad_keep[f, x]
        for o in range(3):
            total = total + grad_last[f, o].astype(F32)
        new = model_t[f] - step[f] * total
        if last:
            model_out[f] = new.T
        else:
            model_t[f] = new
            x_all[f, row] = new.astype(BF16)

    for f in range(freqs):
        gather_x_start(f)
    relayout_v(0)
    gather_x_mid(0)
    relayout_u(0)
    for f in range(freqs):
        observed_t[f] = observed[f].T
    for sweep in range(ITERS):
        last = sweep == ITERS - 1
        gather_x_end(0)
        forward_products(0)
        gather_x_mid(1)
        forward_sums(0)
        start(first_copies(0))
        if sweep == 0:
            relayout_v(1)
            relayout_u(1)
        gather_x_end(1)
        forward_products(1)
        forward_sums(1)
        start(first_copies(1))
        for f in range(freqs):
            first_end(f)
        for f in range(freqs):
            second_end(f, last)
        for f in range(freqs):
            wait(gather_first(f))
            start(gather_second(f))
        if last:
            for f in range(freqs):
                misfit_out[f] = misfit_t[f].T
        wait(gather_second(0))
        backward_products(0)
        backward_sums(0)
        wait(gather_second(1))
        backward_products(1)
        pair_end(0)
        backward_sums(1)
        pair_end(1)
        for f in range(freqs):
            across_end(f, last)
            if not last:
                gather_x_start(f)
        if not last:
            gather_x_mid(0)


def local(u_factors, v_factors, ranks, model_init, observed, step):
    freqs, rows, tile, cols, width = u_factors.shape
    both, share = model_init.shape[2], model_init.shape[1]
    half = both // 2
    raw = (freqs, rows, tile * cols, width)
    vmem = lambda shape, kind: pltpu.VMEM(shape, kind)
    scratch = [
        vmem(raw, BF16), vmem(raw, BF16),
        vmem((freqs, rows, tile, cols * width), BF16), vmem((freqs, cols, tile, rows * width), BF16),
        vmem((tile * cols, width), F32),
        vmem((rows, both, cols * width), BF16), vmem((cols, both, rows * width), BF16),
        vmem((freqs, both, share), F32), vmem((freqs, both, share), F32), vmem((freqs, both, share), F32),
        vmem((freqs, 8, both, share), BF16),
        vmem((freqs, 16, half, share), BF16), vmem((freqs, 16, half, share), BF16),
        vmem((freqs, 3, 4, half, share), BF16), vmem((freqs, 3, 4, half, share), BF16),
        vmem((freqs, 4, half, share), F32), vmem((freqs, 4, half, share), F32),
        vmem((freqs, 4, half, share), BF16), vmem((freqs, 4, half, share), BF16),
        vmem((freqs, 3, half, share), BF16), vmem((freqs, 3, half, share), BF16),
        vmem((freqs, 16, half, share), BF16), vmem((freqs, 16, half, share), BF16),
        vmem((freqs, 2, cols, both, share), F32), vmem((freqs, cols, both, share), F32),
        vmem((freqs, cols, both, share), F32), vmem((freqs, cols, both, share), BF16),
        vmem((freqs, 3, both, share), BF16),
        pltpu.SemaphoreType.DMA((2 * freqs,)),
        pltpu.SemaphoreType.DMA((76,)), pltpu.SemaphoreType.DMA((76,)),
    ]
    in_vmem = pl.BlockSpec(memory_space=pltpu.VMEM)
    in_smem = pl.BlockSpec(memory_space=pltpu.SMEM)
    anywhere = pl.BlockSpec(memory_space=pl.ANY)
    return pl.pallas_call(
        kernel,
        out_shape=(
            jax.ShapeDtypeStruct(model_init.shape, F32), jax.ShapeDtypeStruct(observed.shape, F32),
        ),
        in_specs=[anywhere, anywhere, in_smem, in_vmem, in_vmem, in_smem],
        out_specs=(in_vmem, in_vmem),
        scratch_shapes=scratch,
        compiler_params=pltpu.CompilerParams(
            collective_id=0, has_side_effects=True, vmem_limit_bytes=60 * 2**20
        ),
    )(u_factors.reshape(raw), v_factors.reshape(raw), ranks.reshape(-1), model_init, observed, step)


def solution(mesh):
    return jax.shard_map(
        local,
        mesh=mesh,
        in_specs=(
            P(None, "row", None, "col", None),
            P(None, "row", None, "col", None),
            P(None, "row", "col"),
            P(None, ("col", "row"), None),
            P(None, ("row", "col"), None),
            P(),
        ),
        out_specs=(P(None, ("col", "row"), None), P(None, ("row", "col"), None)),
        check_vma=False,
    )
```

```python
import functools

import jax
import jax.numpy as jnp
from jax import lax
from jax.experimental import pallas as pl
from jax.experimental.pallas import tpu as pltpu
from jax.sharding import PartitionSpec as P

ITERS = 2
MESH = pl.DeviceIdType.MESH
F32, BF16 = jnp.float32, jnp.bfloat16
LANES = 128
TRANS_B = (((1,), (1,)), ((), ()))


def kernel(
    u_hbm, v_hbm, ranks, model_in, observed, step,
    model_out, misfit_out,
    u_raw, v_raw, u_tiles, v_tiles, wide, expanded_f, expanded_b,
    model_t, observed_t, misfit_t,
    x_all, sum_a, sum_b, got_a, got_b, keep_a, keep_b, next_a, next_b, last_a, last_b,
    r_a, r_b, grad, grad_got, grad_keep, grad_send, grad_last,
    load_sem, send_sem, recv_sem,
):
    freqs, rows, cols = u_raw.shape[0], u_raw.shape[1], v_tiles.shape[1]
    tile = v_tiles.shape[2] // 2
    half = x_all.shape[2] // 2
    col, row = lax.axis_index("col"), lax.axis_index("row")
    y, z = col // 4, col % 4
    x, core = row // 2, row % 2

    def at_y(o):
        return ((y + o) % 4 * 4 + z, row)

    def at_z(o):
        return (y * 4 + (z + o) % 4, row)

    def at_x(o):
        return (col, (x + o) % 4 * 2 + core)

    partner = (col, x * 2 + 1 - core)
    numbers = {}

    def remote(name, src, dst, device):
        number = numbers.setdefault(name, len(numbers))
        return pltpu.make_async_remote_copy(
            src_ref=src, dst_ref=dst, send_sem=send_sem.at[number], recv_sem=recv_sem.at[number],
            device_id=device, device_id_type=MESH,
        )

    loads = {}
    for f in range(freqs):
        for n, (src, dst) in enumerate(((v_hbm, v_raw), (u_hbm, u_raw))):
            loads[f, n] = pltpu.make_async_copy(src.at[f], dst.at[f], load_sem.at[2 * f + n])
            loads[f, n].start()

    barrier = pltpu.get_barrier_semaphore()
    peers = [at_y(o) for o in (1, 2, 3)] + [at_z(o) for o in (1, 2, 3)] + [at_x(o) for o in (1, 2, 3)] + [partner]
    for peer in peers:
        pl.semaphore_signal(barrier, inc=1, device_id=peer, device_id_type=MESH)

    for f in range(freqs):
        turned = model_in[f].T
        model_t[f] = turned
        x_all[f, row] = turned.astype(BF16)
    pl.semaphore_wait(barrier, len(peers))

    lane = lax.broadcasted_iota(jnp.int32, (1, LANES), 1)
    low = lane < LANES // 2
    lane_k = lane % (LANES // 2)

    def pick(first, second):
        return jnp.where(low, first, second)

    def swap(value):
        return pltpu.roll(value, LANES // 2, 1)

    def planes(f, raw, p):
        found = []
        for e in range(2):
            wide[e] = raw[f, 2 * p + e].astype(F32)
        for j in range(cols):
            pair = []
            for e in range(2):
                piece = wide[e, pl.ds(j, tile, stride=cols), :]
                pair.append(jnp.where(lane_k < ranks[f, j, 2 * p + e], piece, 0.0))
            found.append(pair)
        return found

    def joined(first, second):
        return pick(first, swap(second)).astype(BF16), pick(swap(first), second).astype(BF16)

    def relayout_v(f):
        loads[f, 0].wait()

        def one(p, carry):
            at = pl.ds(pl.multiple_of(p * LANES, LANES), LANES)
            for j, pair in enumerate(planes(f, v_raw, p)):
                real, imaginary = joined(pair[j % 2], pair[1 - j % 2])
                v_tiles[f, j, :tile, at] = real
                v_tiles[f, j, tile:, at] = imaginary
            return carry

        lax.fori_loop(0, rows // 2, one, 0)

    def relayout_u(f):
        loads[f, 1].wait()

        def one(p, carry):
            found = planes(f, u_raw, p)
            for e in range(2):
                for jp in range(cols // 2):
                    real, imaginary = joined(found[2 * jp + e][e], found[2 * jp + 1 - e][e])
                    u_tiles[f, 2 * p + e, :tile, jp * LANES:(jp + 1) * LANES] = real
                    u_tiles[f, 2 * p + e, tile:, jp * LANES:(jp + 1) * LANES] = imaginary
            return carry

        lax.fori_loop(0, rows // 2, one, 0)

    def gather_x_copies(f):
        own = x_all.at[f, row]
        return [remote(("a", f, o), own, own, at_x(o)) for o in (1, 3, 2)] + [remote(("a", f, 0), own, own, partner)]

    def gather_x_pass(f):
        copies = []
        for o in (1, 3, 2):
            slot = x_all.at[f, (x - o + 4) % 4 * 2 + core]
            copies.append(remote(("ap", f, o), slot, slot, partner))
        return copies

    def gather_x_start(f):
        for copy in gather_x_copies(f):
            copy.start()

    def gather_x_mid(f):
        for copy, onward in zip(gather_x_copies(f)[:3], gather_x_pass(f)):
            copy.wait_recv()
            onward.start()

    def gather_x_end(f):
        copies = gather_x_copies(f)
        copies[3].wait_recv()
        for onward in gather_x_pass(f):
            onward.wait()
        for copy in copies:
            copy.wait_send()

    def adjoint_left(value):
        return jnp.concatenate([value, jnp.concatenate([value[half:], -value[:half]], axis=0)], axis=1)

    def turned_left(value):
        return jnp.concatenate([-value[half:], value[:half]], axis=0)

    def forward_products(f):
        def one(jp, carry):
            lefts = []
            for e in range(2):
                at = 2 * (2 * jp + e)
                lefts.append(adjoint_left(jnp.concatenate([x_all[f, at], x_all[f, at + 1]], axis=1)))
            at = pl.ds(pl.multiple_of(jp * LANES, LANES), LANES)
            for q in range(rows // 4):
                even, odd = (
                    jnp.dot(lefts[e], v_tiles[f, 2 * jp + e, :, q * tile:(q + 1) * tile], preferred_element_type=F32)
                    for e in range(2)
                )
                for p in range(2):
                    one_even, one_odd = even[:, p * LANES:(p + 1) * LANES], odd[:, p * LANES:(p + 1) * LANES]
                    i = 4 * q + 2 * p
                    expanded_f[i, :, at] = pick(one_even, one_odd).astype(BF16)
                    expanded_f[i + 1, :, at] = pick(one_odd, one_even).astype(BF16)
            return carry

        lax.fori_loop(0, cols // 2, one, 0)

    def forward_sums(f):
        def one(i, carry):
            left = expanded_f[i]
            total = lax.dot_general(left, u_tiles[f, i, :tile], TRANS_B, preferred_element_type=F32)
            total = total + lax.dot_general(
                turned_left(left), u_tiles[f, i, tile:], TRANS_B, preferred_element_type=F32
            )
            total = total.astype(BF16)
            for h in range(2):
                part = total[:, h * LANES:(h + 1) * LANES]
                sum_a[f, 2 * i + h] = part[:half]
                sum_b[f, (2 * (i % 2) + h) * 4 + i // 2] = part[half:]
            return carry

        lax.fori_loop(0, rows, one, 0)

    def first_copies(f):
        copies = []
        for o in (2, 1, 3):
            copies.append(remote(("c1a", f, o), sum_a.at[f, pl.ds((y + o) % 4 * 4, 4)], got_a.at[f, o - 1], at_y(o)))
            copies.append(remote(("c1b", f, o), sum_b.at[f, pl.ds((z + o) % 4 * 4, 4)], got_b.at[f, o - 1], at_z(o)))
        return copies

    def second_copies(f):
        copies = []
        for o in (2, 1, 3):
            copies.append(remote(("c2a", f, o), next_a.at[f, (z + o) % 4], last_a.at[f, o - 1], at_z(o)))
            copies.append(remote(("c2b", f, o), next_b.at[f, (y + o) % 4], last_b.at[f, o - 1], at_y(o)))
        return copies

    def start(copies):
        for copy in copies:
            copy.start()

    def wait(copies):
        for copy in copies:
            copy.wait()

    def first_end(f):
        wait(first_copies(f))
        for q in range(4):
            for own, got, keep, onward, at in (
                (sum_a, got_a, keep_a, next_a, y), (sum_b, got_b, keep_b, next_b, z)
            ):
                total = own[f, at * 4 + q].astype(F32)
                for o in range(3):
                    total = total + got[f, o, q].astype(F32)
                keep[f, q] = total
                onward[f, q] = total.astype(BF16)
        start(second_copies(f))

    def gather_first(f):
        copies = []
        own_a, own_b = r_a.at[f, y * 4 + z], r_b.at[f, z * 4 + y]
        for o in (2, 1, 3):
            copies.append(remote(("e1a", f, o), own_a, own_a, at_z(o)))
            copies.append(remote(("e1b", f, o), own_b, own_b, at_y(o)))
        return copies

    def gather_second(f):
        copies = []
        own_a, own_b = r_a.at[f, pl.ds(y * 4, 4)], r_b.at[f, pl.ds(z * 4, 4)]
        for o in (2, 1, 3):
            copies.append(remote(("e2a", f, o), own_a, own_a, at_y(o)))
            copies.append(remote(("e2b", f, o), own_b, own_b, at_z(o)))
        return copies

    def second_end(f, last):
        wait(second_copies(f))
        for keep, got, to, rows_at, at, slot in (
            (keep_a, last_a, r_a, slice(0, half), z, y * 4 + z),
            (keep_b, last_b, r_b, slice(half, tile), y, z * 4 + y),
        ):
            total = keep[f, at]
            for o in range(3):
                total = total + got[f, o].astype(F32)
            total = total - observed_t[f, rows_at]
            if last:
                misfit_t[f, rows_at] = total
            to[f, slot] = total.astype(BF16)
        start(gather_first(f))

    def backward_products(f):
        def one(p, carry):
            found = []
            for e in range(2):
                i = 2 * p + e
                left_a = jnp.concatenate([r_a[f, 2 * i], r_a[f, 2 * i + 1]], axis=1)
                left_b = jnp.concatenate([r_b[f, 8 * e + p], r_b[f, 8 * e + 4 + p]], axis=1)
                left = adjoint_left(jnp.concatenate([left_a, left_b], axis=0))
                found.append(jnp.dot(left, u_tiles[f, i], preferred_element_type=F32))
            at = pl.ds(pl.multiple_of(p * LANES, LANES), LANES)
            for jp in range(cols // 2):
                even, odd = (value[:, jp * LANES:(jp + 1) * LANES] for value in found)
                expanded_b[2 * jp, :, at] = pick(even, odd).astype(BF16)
                expanded_b[2 * jp + 1, :, at] = pick(odd, even).astype(BF16)
            return carry

        lax.fori_loop(0, rows // 2, one, 0)

    def pair_copy(f, j):
        return remote(("g1", f, j), grad.at[f, 1 - core, j], grad_got.at[f, j], partner)

    def backward_sums(f):
        for j in range(cols):
            left = expanded_b[j]
            total = lax.dot_general(left, v_tiles[f, j, :tile], TRANS_B, preferred_element_type=F32)
            total = total + lax.dot_general(
                turned_left(left), v_tiles[f, j, tile:], TRANS_B, preferred_element_type=F32
            )
            for h in range(2):
                grad[f, h, j] = total[:, h * LANES:(h + 1) * LANES]
            pair_copy(f, j).start()

    def across_copies(f):
        return [
            remote(("g2", f, o), grad_send.at[f, (x + o) % 4], grad_last.at[f, o - 1], at_x(o)) for o in (2, 1, 3)
        ]

    def pair_end(f):
        for j in range(cols):
            pair_copy(f, j).wait()
            total = grad[f, core, j] + grad_got[f, j]
            grad_keep[f, j] = total
            grad_send[f, j] = total.astype(BF16)
        start(across_copies(f))

    def across_end(f, last):
        wait(across_copies(f))
        total = grad_keep[f, x]
        for o in range(3):
            total = total + grad_last[f, o].astype(F32)
        new = model_t[f] - step[f] * total
        if last:
            model_out[f] = new.T
        else:
            model_t[f] = new
            x_all[f, row] = new.astype(BF16)

    for f in range(freqs):
        gather_x_start(f)
    relayout_v(0)
    gather_x_mid(0)
    relayout_u(0)
    for f in range(freqs):
        observed_t[f] = observed[f].T
    for sweep in range(ITERS):
        last = sweep == ITERS - 1
        gather_x_end(0)
        forward_products(0)
        gather_x_mid(1)
        forward_sums(0)
        start(first_copies(0))
        if sweep == 0:
            relayout_v(1)
            relayout_u(1)
        gather_x_end(1)
        forward_products(1)
        forward_sums(1)
        start(first_copies(1))
        for f in range(freqs):
            first_end(f)
        for f in range(freqs):
            second_end(f, last)
        for f in range(freqs):
            wait(gather_first(f))
            start(gather_second(f))
        if last:
            for f in range(freqs):
                misfit_out[f] = misfit_t[f].T
        wait(gather_second(0))
        backward_products(0)
        backward_sums(0)
        wait(gather_second(1))
        backward_products(1)
        pair_end(0)
        backward_sums(1)
        pair_end(1)
        for f in range(freqs):
            across_end(f, last)
            if not last:
                gather_x_start(f)
        if not last:
            gather_x_mid(0)


def local(u_factors, v_factors, ranks, model_init, observed, step):
    freqs, rows, tile, cols, width = u_factors.shape
    both, share = model_init.shape[2], model_init.shape[1]
    half = both // 2
    raw = (freqs, rows, tile * cols, width)
    vmem = lambda shape, kind: pltpu.VMEM(shape, kind)
    scratch = [
        vmem(raw, BF16), vmem(raw, BF16),
        vmem((freqs, rows, 2 * tile, cols * width // 2), BF16), vmem((freqs, cols, 2 * tile, rows * width // 2), BF16),
        vmem((2, tile * cols, width), F32),
        vmem((rows, both, cols * width // 2), BF16), vmem((cols, both, rows * width // 2), BF16),
        vmem((freqs, both, share), F32), vmem((freqs, both, share), F32), vmem((freqs, both, share), F32),
        vmem((freqs, 8, both, share), BF16),
        vmem((freqs, 16, half, share), BF16), vmem((freqs, 16, half, share), BF16),
        vmem((freqs, 3, 4, half, share), BF16), vmem((freqs, 3, 4, half, share), BF16),
        vmem((freqs, 4, half, share), F32), vmem((freqs, 4, half, share), F32),
        vmem((freqs, 4, half, share), BF16), vmem((freqs, 4, half, share), BF16),
        vmem((freqs, 3, half, share), BF16), vmem((freqs, 3, half, share), BF16),
        vmem((freqs, 16, half, share), BF16), vmem((freqs, 16, half, share), BF16),
        vmem((freqs, 2, cols, both, share), F32), vmem((freqs, cols, both, share), F32),
        vmem((freqs, cols, both, share), F32), vmem((freqs, cols, both, share), BF16),
        vmem((freqs, 3, both, share), BF16),
        pltpu.SemaphoreType.DMA((2 * freqs,)),
        pltpu.SemaphoreType.DMA((76,)), pltpu.SemaphoreType.DMA((76,)),
    ]
    in_vmem = pl.BlockSpec(memory_space=pltpu.VMEM)
    in_smem = pl.BlockSpec(memory_space=pltpu.SMEM)
    anywhere = pl.BlockSpec(memory_space=pl.ANY)
    return pl.pallas_call(
        kernel,
        out_shape=(
            jax.ShapeDtypeStruct(model_init.shape, F32), jax.ShapeDtypeStruct(observed.shape, F32),
        ),
        in_specs=[anywhere, anywhere, in_smem, in_vmem, in_vmem, in_smem],
        out_specs=(in_vmem, in_vmem),
        scratch_shapes=scratch,
        compiler_params=pltpu.CompilerParams(
            collective_id=0, has_side_effects=True, vmem_limit_bytes=52 * 2**20
        ),
    )(u_factors.reshape(raw), v_factors.reshape(raw), ranks.transpose(0, 2, 1), model_init, observed, step)


def solution(mesh):
    return jax.shard_map(
        local,
        mesh=mesh,
        in_specs=(
            P(None, "row", None, "col", None),
            P(None, "row", None, "col", None),
            P(None, "row", "col"),
            P(None, ("col", "row"), None),
            P(None, ("row", "col"), None),
            P(),
        ),
        out_specs=(P(None, ("col", "row"), None), P(None, ("row", "col"), None)),
        check_vma=False,
    )
```

```python
import functools

import jax
import jax.numpy as jnp
from jax import lax
from jax.experimental import pallas as pl
from jax.experimental.pallas import tpu as pltpu
from jax.sharding import PartitionSpec as P

ITERS = 2
MESH = pl.DeviceIdType.MESH
F32, BF16 = jnp.float32, jnp.bfloat16
LANES = 128
TRANS_B = (((1,), (1,)), ((), ()))
SPLIT = 2
ORDER = (
    0, 1, 2, 3, 0, 1, 0, 1, 2, 3, 2, 3, 0, 1, 2, 3, 0,
    1, 2, 3, 0, 1, 2, 3, 0, 1, 0, 2, 1, 3, 0, 2, 1, 3,
    0, 2, 0, 1, 3, 1, 2, 2, 0, 3, 3, 1, 2, 0, 3, 1, 2,
    0, 3, 1, 2, 0, 3, 0, 1, 2, 1, 0, 3, 2, 1, 3, 2, 3,
)


def kernel(
    u_hbm, v_hbm, ranks, model_in, observed, step,
    model_out, misfit_out,
    u_raw, v_raw, u_tiles, v_tiles, wide, expanded_f, expanded_b,
    model_t, observed_t, misfit_t,
    x_all, sum_a, sum_b, got_a, got_b, keep_a, keep_b, next_a, next_b, last_a, last_b,
    r_a, r_b, grad, grad_got, grad_keep, grad_send, grad_last,
    load_sem, send_sem, recv_sem,
):
    freqs, rows, cols = u_raw.shape[0], u_raw.shape[1], v_tiles.shape[1]
    chains = freqs * SPLIT
    tile = v_tiles.shape[2] // 2
    half = x_all.shape[2] // 2
    col, row = lax.axis_index("col"), lax.axis_index("row")
    y, z = col // 4, col % 4
    x, core = row // 2, row % 2

    def at_y(o):
        return ((y + o) % 4 * 4 + z, row)

    def at_z(o):
        return (y * 4 + (z + o) % 4, row)

    def at_x(o):
        return (col, (x + o) % 4 * 2 + core)

    partner = (col, x * 2 + 1 - core)
    numbers = {}

    def remote(name, src, dst, device):
        number = numbers.setdefault(name, len(numbers))
        return pltpu.make_async_remote_copy(
            src_ref=src, dst_ref=dst, send_sem=send_sem.at[number], recv_sem=recv_sem.at[number],
            device_id=device, device_id_type=MESH,
        )

    loads = {}
    for f in range(freqs):
        for n, (src, dst) in enumerate(((v_hbm, v_raw), (u_hbm, u_raw))):
            loads[f, n] = pltpu.make_async_copy(src.at[f], dst.at[f], load_sem.at[2 * f + n])
            loads[f, n].start()

    barrier = pltpu.get_barrier_semaphore()
    peers = [at_y(o) for o in (1, 2, 3)] + [at_z(o) for o in (1, 2, 3)] + [at_x(o) for o in (1, 2, 3)] + [partner]
    for peer in peers:
        pl.semaphore_signal(barrier, inc=1, device_id=peer, device_id_type=MESH)

    def chain_rows(f, turned):
        full = turned.shape[0] // 2
        return [
            (SPLIT * f + h, jnp.concatenate([turned[b + h * half:b + (h + 1) * half] for b in (0, full)], axis=0))
            for h in range(SPLIT)
        ]

    def whole_rows(f, ref):
        parts = [ref[SPLIT * f + h] for h in range(SPLIT)]
        return jnp.concatenate([part[:half] for part in parts] + [part[half:] for part in parts], axis=0).T

    for f in range(freqs):
        for c, turned in chain_rows(f, model_in[f].T):
            model_t[c] = turned
            x_all[c, row] = turned.astype(BF16)
    pl.semaphore_wait(barrier, len(peers))

    lane = lax.broadcasted_iota(jnp.int32, (1, LANES), 1)
    low = lane < LANES // 2
    lane_k = lane % (LANES // 2)

    def pick(first, second):
        return jnp.where(low, first, second)

    def swap(value):
        return pltpu.roll(value, LANES // 2, 1)

    def planes(f, raw, p):
        found = []
        for e in range(2):
            wide[e] = raw[f, 2 * p + e].astype(F32)
        for j in range(cols):
            pair = []
            for e in range(2):
                piece = wide[e, pl.ds(j, tile, stride=cols), :]
                pair.append(jnp.where(lane_k < ranks[f, j, 2 * p + e], piece, 0.0))
            found.append(pair)
        return found

    def joined(first, second):
        return pick(first, swap(second)).astype(BF16), pick(swap(first), second).astype(BF16)

    def relayout_v(f):
        loads[f, 0].wait()

        def one(p, carry):
            at = pl.ds(pl.multiple_of(p * LANES, LANES), LANES)
            for j, pair in enumerate(planes(f, v_raw, p)):
                real, imaginary = joined(pair[j % 2], pair[1 - j % 2])
                v_tiles[f, j, :tile, at] = real
                v_tiles[f, j, tile:, at] = imaginary
            return carry

        lax.fori_loop(0, rows // 2, one, 0)

    def relayout_u(f):
        loads[f, 1].wait()

        def one(p, carry):
            found = planes(f, u_raw, p)
            for e in range(2):
                for jp in range(cols // 2):
                    real, imaginary = joined(found[2 * jp + e][e], found[2 * jp + 1 - e][e])
                    u_tiles[f, 2 * p + e, :tile, jp * LANES:(jp + 1) * LANES] = real
                    u_tiles[f, 2 * p + e, tile:, jp * LANES:(jp + 1) * LANES] = imaginary
            return carry

        lax.fori_loop(0, rows // 2, one, 0)

    def gather_x_copies(f):
        own = x_all.at[f, row]
        return [remote(("a", f, o), own, own, at_x(o)) for o in (1, 3, 2)] + [remote(("a", f, 0), own, own, partner)]

    def gather_x_pass(f):
        copies = []
        for o in (1, 3, 2):
            slot = x_all.at[f, (x - o + 4) % 4 * 2 + core]
            copies.append(remote(("ap", f, o), slot, slot, partner))
        return copies

    def gather_x_start(f):
        for copy in gather_x_copies(f):
            copy.start()

    def gather_x_mid(f):
        for copy, onward in zip(gather_x_copies(f)[:3], gather_x_pass(f)):
            copy.wait_recv()
            onward.start()

    def gather_x_end(f):
        copies = gather_x_copies(f)
        copies[3].wait_recv()
        for onward in gather_x_pass(f):
            onward.wait()
        for copy in copies:
            copy.wait_send()

    def adjoint_left(value):
        return jnp.concatenate([value, jnp.concatenate([value[half:], -value[:half]], axis=0)], axis=1)

    def turned_left(value):
        return jnp.concatenate([-value[half:], value[:half]], axis=0)

    def forward_products(f):
        for jp in range(cols // 2):
            lefts = []
            for e in range(2):
                at = 2 * (2 * jp + e)
                lefts.append(adjoint_left(jnp.concatenate([x_all[f, at], x_all[f, at + 1]], axis=1)))
            for q in range(rows // 4):
                even, odd = (
                    jnp.dot(
                        lefts[e], v_tiles[f // SPLIT, 2 * jp + e, :, q * tile:(q + 1) * tile],
                        preferred_element_type=F32,
                    )
                    for e in range(2)
                )
                for p in range(2):
                    one_even, one_odd = even[:, p * LANES:(p + 1) * LANES], odd[:, p * LANES:(p + 1) * LANES]
                    i = 4 * q + 2 * p
                    expanded_f[i, :, jp * LANES:(jp + 1) * LANES] = pick(one_even, one_odd).astype(BF16)
                    expanded_f[i + 1, :, jp * LANES:(jp + 1) * LANES] = pick(one_odd, one_even).astype(BF16)

    def forward_sums(f):
        for i in range(rows):
            left = expanded_f[i]
            total = lax.dot_general(left, u_tiles[f // SPLIT, i, :tile], TRANS_B, preferred_element_type=F32)
            total = total + lax.dot_general(
                turned_left(left), u_tiles[f // SPLIT, i, tile:], TRANS_B, preferred_element_type=F32
            )
            total = total.astype(BF16)
            for h in range(2):
                part = total[:, h * LANES:(h + 1) * LANES]
                sum_a[f, 2 * i + h] = part[:half]
                sum_b[f, (2 * (i % 2) + h) * 4 + i // 2] = part[half:]

    def first_copies(f):
        copies = []
        for o in (2, 1, 3):
            copies.append(remote(("c1a", f, o), sum_a.at[f, pl.ds((y + o) % 4 * 4, 4)], got_a.at[f, o - 1], at_y(o)))
            copies.append(remote(("c1b", f, o), sum_b.at[f, pl.ds((z + o) % 4 * 4, 4)], got_b.at[f, o - 1], at_z(o)))
        return copies

    def second_copies(f):
        copies = []
        for o in (2, 1, 3):
            copies.append(remote(("c2a", f, o), next_a.at[f, (z + o) % 4], last_a.at[f, o - 1], at_z(o)))
            copies.append(remote(("c2b", f, o), next_b.at[f, (y + o) % 4], last_b.at[f, o - 1], at_y(o)))
        return copies

    def start(copies):
        for copy in copies:
            copy.start()

    def wait(copies):
        for copy in copies:
            copy.wait()

    def first_end(f):
        wait(first_copies(f))
        for q in range(4):
            for own, got, keep, onward, at in (
                (sum_a, got_a, keep_a, next_a, y), (sum_b, got_b, keep_b, next_b, z)
            ):
                total = own[f, at * 4 + q].astype(F32)
                for o in range(3):
                    total = total + got[f, o, q].astype(F32)
                keep[f, q] = total
                onward[f, q] = total.astype(BF16)
        start(second_copies(f))

    def gather_first(f):
        copies = []
        own_a, own_b = r_a.at[f, y * 4 + z], r_b.at[f, z * 4 + y]
        for o in (2, 1, 3):
            copies.append(remote(("e1a", f, o), own_a, own_a, at_z(o)))
            copies.append(remote(("e1b", f, o), own_b, own_b, at_y(o)))
        return copies

    def gather_second(f):
        copies = []
        own_a, own_b = r_a.at[f, pl.ds(y * 4, 4)], r_b.at[f, pl.ds(z * 4, 4)]
        for o in (2, 1, 3):
            copies.append(remote(("e2a", f, o), own_a, own_a, at_y(o)))
            copies.append(remote(("e2b", f, o), own_b, own_b, at_z(o)))
        return copies

    def second_end(f, last):
        wait(second_copies(f))
        for keep, got, to, rows_at, at, slot in (
            (keep_a, last_a, r_a, slice(0, half), z, y * 4 + z),
            (keep_b, last_b, r_b, slice(half, tile), y, z * 4 + y),
        ):
            total = keep[f, at]
            for o in range(3):
                total = total + got[f, o].astype(F32)
            total = total - observed_t[f, rows_at]
            if last:
                misfit_t[f, rows_at] = total
            to[f, slot] = total.astype(BF16)
        start(gather_first(f))

    def backward_products(f):
        for p in range(rows // 2):
            found = []
            for e in range(2):
                i = 2 * p + e
                left_a = jnp.concatenate([r_a[f, 2 * i], r_a[f, 2 * i + 1]], axis=1)
                left_b = jnp.concatenate([r_b[f, 8 * e + p], r_b[f, 8 * e + 4 + p]], axis=1)
                left = adjoint_left(jnp.concatenate([left_a, left_b], axis=0))
                found.append(jnp.dot(left, u_tiles[f // SPLIT, i], preferred_element_type=F32))
            for jp in range(cols // 2):
                even, odd = (value[:, jp * LANES:(jp + 1) * LANES] for value in found)
                expanded_b[2 * jp, :, p * LANES:(p + 1) * LANES] = pick(even, odd).astype(BF16)
                expanded_b[2 * jp + 1, :, p * LANES:(p + 1) * LANES] = pick(odd, even).astype(BF16)

    def pair_copy(f, j):
        return remote(("g1", f, j), grad.at[f, 1 - core, j], grad_got.at[f, j], partner)

    def backward_sums(f):
        for j in range(cols):
            left = expanded_b[j]
            total = lax.dot_general(left, v_tiles[f // SPLIT, j, :tile], TRANS_B, preferred_element_type=F32)
            total = total + lax.dot_general(
                turned_left(left), v_tiles[f // SPLIT, j, tile:], TRANS_B, preferred_element_type=F32
            )
            for h in range(2):
                grad[f, h, j] = total[:, h * LANES:(h + 1) * LANES]
            pair_copy(f, j).start()

    def across_copies(f):
        return [
            remote(("g2", f, o), grad_send.at[f, (x + o) % 4], grad_last.at[f, o - 1], at_x(o)) for o in (2, 1, 3)
        ]

    def pair_end(f):
        for j in range(cols):
            pair_copy(f, j).wait()
            total = grad[f, core, j] + grad_got[f, j]
            grad_keep[f, j] = total
            grad_send[f, j] = total.astype(BF16)
        start(across_copies(f))

    def across_end(f, last):
        wait(across_copies(f))
        total = grad_keep[f, x]
        for o in range(3):
            total = total + grad_last[f, o].astype(F32)
        new = model_t[f] - step[f // SPLIT] * total
        model_t[f] = new
        if not last:
            x_all[f, row] = new.astype(BF16)
            gather_x_start(f)

    def stages(f):
        gather_x_start(f)
        yield
        for sweep in range(ITERS):
            last = sweep == ITERS - 1
            gather_x_mid(f)
            yield
            if sweep == 0 and f % SPLIT == 0:
                relayout_v(f // SPLIT)
                relayout_u(f // SPLIT)
                for c, turned in chain_rows(f // SPLIT, observed[f // SPLIT].T):
                    observed_t[c] = turned
            gather_x_end(f)
            forward_products(f)
            forward_sums(f)
            start(first_copies(f))
            yield
            first_end(f)
            yield
            second_end(f, last)
            yield
            wait(gather_first(f))
            start(gather_second(f))
            if last and f % SPLIT == SPLIT - 1:
                misfit_out[f // SPLIT] = whole_rows(f // SPLIT, misfit_t)
            yield
            wait(gather_second(f))
            backward_products(f)
            backward_sums(f)
            yield
            pair_end(f)
            yield
            across_end(f, last)
            if last and f % SPLIT == SPLIT - 1:
                model_out[f // SPLIT] = whole_rows(f // SPLIT, model_t)
            yield

    running = [stages(f) for f in range(chains)]
    for f in ORDER:
        next(running[f])


def local(u_factors, v_factors, ranks, model_init, observed, step):
    freqs, rows, tile, cols, width = u_factors.shape
    both, share = model_init.shape[2], model_init.shape[1]
    chains, part = freqs * SPLIT, both // SPLIT
    half = part // 2
    raw = (freqs, rows, tile * cols, width)
    vmem = lambda shape, kind: pltpu.VMEM(shape, kind)
    scratch = [
        vmem(raw, BF16), vmem(raw, BF16),
        vmem((freqs, rows, 2 * tile, cols * width // 2), BF16), vmem((freqs, cols, 2 * tile, rows * width // 2), BF16),
        vmem((2, tile * cols, width), F32),
        vmem((rows, part, cols * width // 2), BF16), vmem((cols, part, rows * width // 2), BF16),
        vmem((chains, part, share), F32), vmem((chains, part, share), F32), vmem((chains, part, share), F32),
        vmem((chains, 8, part, share), BF16),
        vmem((chains, 16, half, share), BF16), vmem((chains, 16, half, share), BF16),
        vmem((chains, 3, 4, half, share), BF16), vmem((chains, 3, 4, half, share), BF16),
        vmem((chains, 4, half, share), F32), vmem((chains, 4, half, share), F32),
        vmem((chains, 4, half, share), BF16), vmem((chains, 4, half, share), BF16),
        vmem((chains, 3, half, share), BF16), vmem((chains, 3, half, share), BF16),
        vmem((chains, 16, half, share), BF16), vmem((chains, 16, half, share), BF16),
        vmem((chains, 2, cols, part, share), F32), vmem((chains, cols, part, share), F32),
        vmem((chains, cols, part, share), F32), vmem((chains, cols, part, share), BF16),
        vmem((chains, 3, part, share), BF16),
        pltpu.SemaphoreType.DMA((2 * freqs,)),
        pltpu.SemaphoreType.DMA((38 * chains,)), pltpu.SemaphoreType.DMA((38 * chains,)),
    ]
    in_vmem = pl.BlockSpec(memory_space=pltpu.VMEM)
    in_smem = pl.BlockSpec(memory_space=pltpu.SMEM)
    anywhere = pl.BlockSpec(memory_space=pl.ANY)
    return pl.pallas_call(
        kernel,
        out_shape=(
            jax.ShapeDtypeStruct(model_init.shape, F32), jax.ShapeDtypeStruct(observed.shape, F32),
        ),
        in_specs=[anywhere, anywhere, in_smem, in_vmem, in_vmem, in_smem],
        out_specs=(in_vmem, in_vmem),
        scratch_shapes=scratch,
        compiler_params=pltpu.CompilerParams(
            collective_id=0, has_side_effects=True, vmem_limit_bytes=52 * 2**20
        ),
    )(u_factors.reshape(raw), v_factors.reshape(raw), ranks.transpose(0, 2, 1), model_init, observed, step)


def solution(mesh):
    return jax.shard_map(
        local,
        mesh=mesh,
        in_specs=(
            P(None, "row", None, "col", None),
            P(None, "row", None, "col", None),
            P(None, "row", "col"),
            P(None, ("col", "row"), None),
            P(None, ("row", "col"), None),
            P(),
        ),
        out_specs=(P(None, ("col", "row"), None), P(None, ("row", "col"), None)),
        check_vma=False,
    )
```

```python
import functools

import jax
import jax.numpy as jnp
from jax import lax
from jax.experimental import pallas as pl
from jax.experimental.pallas import tpu as pltpu
from jax.sharding import PartitionSpec as P

ITERS = 2
MESH = pl.DeviceIdType.MESH
F32, BF16 = jnp.float32, jnp.bfloat16
LANES = 128
TRANS_B = (((1,), (1,)), ((), ()))
SPLIT = 2
ORDER = (
    0, 1, 2, 3, 0, 0, 2, 2, 3, 1, 0, 3, 2, 0, 1, 2, 3,
    0, 1, 3, 2, 0, 1, 3, 0, 2, 1, 2, 0, 3, 3, 1, 2, 0,
    1, 0, 3, 2, 2, 1, 3, 0, 3, 1, 2, 0, 1, 3, 2, 0, 1,
    3, 2, 1, 3, 0, 1, 2, 0, 3, 2, 1, 0, 3, 1, 2, 3, 1,
)


def kernel(
    u_hbm, v_hbm, ranks, model_hbm, observed_hbm, step,
    model_out, misfit_out,
    model_in, observed, u_raw, v_raw, u_tiles, v_tiles, wide, expanded_f, expanded_b,
    model_t, observed_t, misfit_t,
    x_all, sum_a, sum_b, got_a, got_b, keep_a, keep_b, next_a, next_b, last_a, last_b,
    r_a, r_b, grad, grad_got, grad_keep, grad_send, grad_last,
    load_sem, send_sem, recv_sem,
):
    freqs, rows, cols = u_raw.shape[0], u_raw.shape[1], v_tiles.shape[1]
    chains = freqs * SPLIT
    tile = v_tiles.shape[2] // 2
    half = x_all.shape[2] // 2
    col, row = lax.axis_index("col"), lax.axis_index("row")
    y, z = col // 4, col % 4
    x, core = row // 2, row % 2

    def at_y(o):
        return ((y + o) % 4 * 4 + z, row)

    def at_z(o):
        return (y * 4 + (z + o) % 4, row)

    def at_x(o):
        return (col, (x + o) % 4 * 2 + core)

    partner = (col, x * 2 + 1 - core)
    numbers = {}

    def remote(name, src, dst, device):
        number = numbers.setdefault(name, len(numbers))
        return pltpu.make_async_remote_copy(
            src_ref=src, dst_ref=dst, send_sem=send_sem.at[number], recv_sem=recv_sem.at[number],
            device_id=device, device_id_type=MESH,
        )

    side_loads = [
        pltpu.make_async_copy(src, dst, load_sem.at[2 * freqs + n])
        for n, (src, dst) in enumerate(((model_hbm, model_in), (observed_hbm, observed)))
    ]
    side_loads[0].start()
    loads = {}
    for f in range(freqs):
        for n, (src, dst) in enumerate(((v_hbm, v_raw), (u_hbm, u_raw))):
            loads[f, n] = pltpu.make_async_copy(src.at[f], dst.at[f], load_sem.at[2 * f + n])
            loads[f, n].start()

    side_loads[1].start()
    barrier = pltpu.get_barrier_semaphore()
    peers = [at_y(o) for o in (1, 2, 3)] + [at_z(o) for o in (1, 2, 3)] + [at_x(o) for o in (1, 2, 3)] + [partner]
    for peer in peers:
        pl.semaphore_signal(barrier, inc=1, device_id=peer, device_id_type=MESH)

    def chain_rows(f, turned):
        full = turned.shape[0] // 2
        return [
            (SPLIT * f + h, jnp.concatenate([turned[b + h * half:b + (h + 1) * half] for b in (0, full)], axis=0))
            for h in range(SPLIT)
        ]

    def whole_rows(f, ref):
        parts = [ref[SPLIT * f + h] for h in range(SPLIT)]
        return jnp.concatenate([part[:half] for part in parts] + [part[half:] for part in parts], axis=0).T

    side_loads[0].wait()
    for f in range(freqs):
        for c, turned in chain_rows(f, model_in[f].T):
            model_t[c] = turned
            x_all[c, row] = turned.astype(BF16)
    pl.semaphore_wait(barrier, len(peers))

    lane = lax.broadcasted_iota(jnp.int32, (1, LANES), 1)
    low = lane < LANES // 2
    lane_k = lane % (LANES // 2)

    def pick(first, second):
        return jnp.where(low, first, second)

    def swap(value):
        return pltpu.roll(value, LANES // 2, 1)

    def planes(f, raw, p):
        found = []
        for e in range(2):
            wide[e] = raw[f, 2 * p + e].astype(F32)
        for j in range(cols):
            pair = []
            for e in range(2):
                piece = wide[e, pl.ds(j, tile, stride=cols), :]
                pair.append(jnp.where(lane_k < ranks[f, j, 2 * p + e], piece, 0.0))
            found.append(pair)
        return found

    def joined(first, second):
        return pick(first, swap(second)).astype(BF16), pick(swap(first), second).astype(BF16)

    def relayout_v(f):
        loads[f, 0].wait()

        def one(p, carry):
            at = pl.ds(pl.multiple_of(p * LANES, LANES), LANES)
            for j, pair in enumerate(planes(f, v_raw, p)):
                real, imaginary = joined(pair[j % 2], pair[1 - j % 2])
                v_tiles[f, j, :tile, at] = real
                v_tiles[f, j, tile:, at] = imaginary
            return carry

        lax.fori_loop(0, rows // 2, one, 0)

    def relayout_u(f):
        loads[f, 1].wait()

        def one(p, carry):
            found = planes(f, u_raw, p)
            for e in range(2):
                for jp in range(cols // 2):
                    real, imaginary = joined(found[2 * jp + e][e], found[2 * jp + 1 - e][e])
                    u_tiles[f, 2 * p + e, :tile, jp * LANES:(jp + 1) * LANES] = real
                    u_tiles[f, 2 * p + e, tile:, jp * LANES:(jp + 1) * LANES] = imaginary
            return carry

        lax.fori_loop(0, rows // 2, one, 0)

    def gather_x_copies(f):
        own = x_all.at[f, row]
        return [remote(("a", f, o), own, own, at_x(o)) for o in (1, 3, 2)] + [remote(("a", f, 0), own, own, partner)]

    def gather_x_pass(f):
        copies = []
        for o in (1, 3, 2):
            slot = x_all.at[f, (x - o + 4) % 4 * 2 + core]
            copies.append(remote(("ap", f, o), slot, slot, partner))
        return copies

    def gather_x_start(f):
        for copy in gather_x_copies(f):
            copy.start()

    def gather_x_mid(f):
        for copy, onward in zip(gather_x_copies(f)[:3], gather_x_pass(f)):
            copy.wait_recv()
            onward.start()

    def gather_x_end(f):
        copies = gather_x_copies(f)
        copies[3].wait_recv()
        for onward in gather_x_pass(f):
            onward.wait()
        for copy in copies:
            copy.wait_send()

    def adjoint_left(value):
        return jnp.concatenate([value, jnp.concatenate([value[half:], -value[:half]], axis=0)], axis=1)

    def turned_left(value):
        return jnp.concatenate([-value[half:], value[:half]], axis=0)

    def forward_products(f):
        for jp in range(cols // 2):
            lefts = []
            for e in range(2):
                at = 2 * (2 * jp + e)
                lefts.append(adjoint_left(jnp.concatenate([x_all[f, at], x_all[f, at + 1]], axis=1)))
            for q in range(rows // 4):
                even, odd = (
                    jnp.dot(
                        lefts[e], v_tiles[f // SPLIT, 2 * jp + e, :, q * tile:(q + 1) * tile],
                        preferred_element_type=F32,
                    )
                    for e in range(2)
                )
                for p in range(2):
                    one_even, one_odd = even[:, p * LANES:(p + 1) * LANES], odd[:, p * LANES:(p + 1) * LANES]
                    i = 4 * q + 2 * p
                    expanded_f[i, :, jp * LANES:(jp + 1) * LANES] = pick(one_even, one_odd).astype(BF16)
                    expanded_f[i + 1, :, jp * LANES:(jp + 1) * LANES] = pick(one_odd, one_even).astype(BF16)

    def forward_sums(f):
        for i in range(rows):
            left = expanded_f[i]
            total = lax.dot_general(left, u_tiles[f // SPLIT, i, :tile], TRANS_B, preferred_element_type=F32)
            total = total + lax.dot_general(
                turned_left(left), u_tiles[f // SPLIT, i, tile:], TRANS_B, preferred_element_type=F32
            )
            total = total.astype(BF16)
            for h in range(2):
                part = total[:, h * LANES:(h + 1) * LANES]
                sum_a[f, 2 * i + h] = part[:half]
                sum_b[f, (2 * (i % 2) + h) * 4 + i // 2] = part[half:]

    def first_copies(f):
        copies = []
        for o in (2, 1, 3):
            copies.append(remote(("c1a", f, o), sum_a.at[f, pl.ds((y + o) % 4 * 4, 4)], got_a.at[f, o - 1], at_y(o)))
            copies.append(remote(("c1b", f, o), sum_b.at[f, pl.ds((z + o) % 4 * 4, 4)], got_b.at[f, o - 1], at_z(o)))
        return copies

    def second_copies(f):
        copies = []
        for o in (2, 1, 3):
            copies.append(remote(("c2a", f, o), next_a.at[f, (z + o) % 4], last_a.at[f, o - 1], at_z(o)))
            copies.append(remote(("c2b", f, o), next_b.at[f, (y + o) % 4], last_b.at[f, o - 1], at_y(o)))
        return copies

    def start(copies):
        for copy in copies:
            copy.start()

    def wait(copies):
        for copy in copies:
            copy.wait()

    def first_end(f):
        wait(first_copies(f))
        for q in range(4):
            for own, got, keep, onward, at in (
                (sum_a, got_a, keep_a, next_a, y), (sum_b, got_b, keep_b, next_b, z)
            ):
                total = own[f, at * 4 + q].astype(F32)
                for o in range(3):
                    total = total + got[f, o, q].astype(F32)
                keep[f, q] = total
                onward[f, q] = total.astype(BF16)
        start(second_copies(f))

    def gather_first(f):
        copies = []
        own_a, own_b = r_a.at[f, y * 4 + z], r_b.at[f, z * 4 + y]
        for o in (2, 1, 3):
            copies.append(remote(("e1a", f, o), own_a, own_a, at_z(o)))
            copies.append(remote(("e1b", f, o), own_b, own_b, at_y(o)))
        return copies

    def gather_second(f):
        copies = []
        own_a, own_b = r_a.at[f, pl.ds(y * 4, 4)], r_b.at[f, pl.ds(z * 4, 4)]
        for o in (2, 1, 3):
            copies.append(remote(("e2a", f, o), own_a, own_a, at_y(o)))
            copies.append(remote(("e2b", f, o), own_b, own_b, at_z(o)))
        return copies

    def second_end(f, last):
        wait(second_copies(f))
        for keep, got, to, rows_at, at, slot in (
            (keep_a, last_a, r_a, slice(0, half), z, y * 4 + z),
            (keep_b, last_b, r_b, slice(half, tile), y, z * 4 + y),
        ):
            total = keep[f, at]
            for o in range(3):
                total = total + got[f, o].astype(F32)
            total = total - observed_t[f, rows_at]
            if last:
                misfit_t[f, rows_at] = total
            to[f, slot] = total.astype(BF16)
        start(gather_first(f))

    def backward_products(f):
        for p in range(rows // 2):
            found = []
            for e in range(2):
                i = 2 * p + e
                left_a = jnp.concatenate([r_a[f, 2 * i], r_a[f, 2 * i + 1]], axis=1)
                left_b = jnp.concatenate([r_b[f, 8 * e + p], r_b[f, 8 * e + 4 + p]], axis=1)
                left = adjoint_left(jnp.concatenate([left_a, left_b], axis=0))
                found.append(jnp.dot(left, u_tiles[f // SPLIT, i], preferred_element_type=F32))
            for jp in range(cols // 2):
                even, odd = (value[:, jp * LANES:(jp + 1) * LANES] for value in found)
                expanded_b[2 * jp, :, p * LANES:(p + 1) * LANES] = pick(even, odd).astype(BF16)
                expanded_b[2 * jp + 1, :, p * LANES:(p + 1) * LANES] = pick(odd, even).astype(BF16)

    def pair_copy(f, j):
        return remote(("g1", f, j), grad.at[f, 1 - core, j], grad_got.at[f, j], partner)

    def backward_sums(f):
        for j in range(cols):
            left = expanded_b[j]
            total = lax.dot_general(left, v_tiles[f // SPLIT, j, :tile], TRANS_B, preferred_element_type=F32)
            total = total + lax.dot_general(
                turned_left(left), v_tiles[f // SPLIT, j, tile:], TRANS_B, preferred_element_type=F32
            )
            for h in range(2):
                grad[f, h, j] = total[:, h * LANES:(h + 1) * LANES]
            pair_copy(f, j).start()

    def across_copies(f):
        return [
            remote(("g2", f, o), grad_send.at[f, (x + o) % 4], grad_last.at[f, o - 1], at_x(o)) for o in (2, 1, 3)
        ]

    def pair_end(f):
        for j in range(cols):
            pair_copy(f, j).wait()
            total = grad[f, core, j] + grad_got[f, j]
            grad_keep[f, j] = total
            grad_send[f, j] = total.astype(BF16)
        start(across_copies(f))

    def across_end(f, last):
        wait(across_copies(f))
        total = grad_keep[f, x]
        for o in range(3):
            total = total + grad_last[f, o].astype(F32)
        new = model_t[f] - step[f // SPLIT] * total
        model_t[f] = new
        if not last:
            x_all[f, row] = new.astype(BF16)
            gather_x_start(f)

    def prepare(f):
        relayout_v(f)
        relayout_u(f)
        if f == 0:
            side_loads[1].wait()
        for c, turned in chain_rows(f, observed[f].T):
            observed_t[c] = turned

    def stages(f):
        gather_x_start(f)
        if f == chains - 1:
            prepare(0)
        yield
        for sweep in range(ITERS):
            last = sweep == ITERS - 1
            gather_x_mid(f)
            yield
            if sweep == 0 and f % SPLIT == 0 and f > 0:
                prepare(f // SPLIT)
            gather_x_end(f)
            forward_products(f)
            forward_sums(f)
            start(first_copies(f))
            yield
            first_end(f)
            yield
            second_end(f, last)
            yield
            wait(gather_first(f))
            start(gather_second(f))
            if last and f % SPLIT == SPLIT - 1:
                misfit_out[f // SPLIT] = whole_rows(f // SPLIT, misfit_t)
            yield
            wait(gather_second(f))
            backward_products(f)
            backward_sums(f)
            yield
            pair_end(f)
            yield
            across_end(f, last)
            if last and f % SPLIT == SPLIT - 1:
                model_out[f // SPLIT] = whole_rows(f // SPLIT, model_t)
            yield

    running = [stages(f) for f in range(chains)]
    for f in ORDER:
        next(running[f])


def local(u_factors, v_factors, ranks, model_init, observed, step):
    freqs, rows, tile, cols, width = u_factors.shape
    both, share = model_init.shape[2], model_init.shape[1]
    chains, part = freqs * SPLIT, both // SPLIT
    half = part // 2
    raw = (freqs, rows, tile * cols, width)
    vmem = lambda shape, kind: pltpu.VMEM(shape, kind)
    scratch = [
        vmem(model_init.shape, F32), vmem(observed.shape, F32), vmem(raw, BF16), vmem(raw, BF16),
        vmem((freqs, rows, 2 * tile, cols * width // 2), BF16), vmem((freqs, cols, 2 * tile, rows * width // 2), BF16),
        vmem((2, tile * cols, width), F32),
        vmem((rows, part, cols * width // 2), BF16), vmem((cols, part, rows * width // 2), BF16),
        vmem((chains, part, share), F32), vmem((chains, part, share), F32), vmem((chains, part, share), F32),
        vmem((chains, 8, part, share), BF16),
        vmem((chains, 16, half, share), BF16), vmem((chains, 16, half, share), BF16),
        vmem((chains, 3, 4, half, share), BF16), vmem((chains, 3, 4, half, share), BF16),
        vmem((chains, 4, half, share), F32), vmem((chains, 4, half, share), F32),
        vmem((chains, 4, half, share), BF16), vmem((chains, 4, half, share), BF16),
        vmem((chains, 3, half, share), BF16), vmem((chains, 3, half, share), BF16),
        vmem((chains, 16, half, share), BF16), vmem((chains, 16, half, share), BF16),
        vmem((chains, 2, cols, part, share), F32), vmem((chains, cols, part, share), F32),
        vmem((chains, cols, part, share), F32), vmem((chains, cols, part, share), BF16),
        vmem((chains, 3, part, share), BF16),
        pltpu.SemaphoreType.DMA((2 * freqs + 2,)),
        pltpu.SemaphoreType.DMA((38 * chains,)), pltpu.SemaphoreType.DMA((38 * chains,)),
    ]
    in_vmem = pl.BlockSpec(memory_space=pltpu.VMEM)
    in_smem = pl.BlockSpec(memory_space=pltpu.SMEM)
    anywhere = pl.BlockSpec(memory_space=pl.ANY)
    return pl.pallas_call(
        kernel,
        out_shape=(
            jax.ShapeDtypeStruct(model_init.shape, F32), jax.ShapeDtypeStruct(observed.shape, F32),
        ),
        in_specs=[anywhere, anywhere, in_smem, anywhere, anywhere, in_smem],
        out_specs=(in_vmem, in_vmem),
        scratch_shapes=scratch,
        compiler_params=pltpu.CompilerParams(
            collective_id=0, has_side_effects=True, vmem_limit_bytes=int(53.25 * 2**20)
        ),
    )(u_factors.reshape(raw), v_factors.reshape(raw), ranks.transpose(0, 2, 1), model_init, observed, step)


def solution(mesh):
    return jax.shard_map(
        local,
        mesh=mesh,
        in_specs=(
            P(None, "row", None, "col", None),
            P(None, "row", None, "col", None),
            P(None, "row", "col"),
            P(None, ("col", "row"), None),
            P(None, ("row", "col"), None),
            P(),
        ),
        out_specs=(P(None, ("col", "row"), None), P(None, ("row", "col"), None)),
        check_vma=False,
    )
```

```python
import functools

import jax
import jax.numpy as jnp
from jax import lax
from jax.experimental import pallas as pl
from jax.experimental.pallas import tpu as pltpu
from jax.sharding import PartitionSpec as P

ITERS = 2
MESH = pl.DeviceIdType.MESH
F32, BF16 = jnp.float32, jnp.bfloat16
LANES = 128
TRANS_B = (((1,), (1,)), ((), ()))
SPLIT = 2
ORDER = (
    0, 1, 2, 3, 0, 0, 2, 2, 3, 1, 0, 3, 2, 0, 1, 2, 3,
    0, 1, 3, 2, 0, 1, 3, 0, 2, 1, 2, 0, 3, 3, 1, 2, 0,
    1, 0, 3, 2, 2, 1, 3, 0, 3, 1, 2, 0, 1, 3, 2, 0, 1,
    3, 2, 1, 3, 0, 1, 2, 0, 3, 2, 1, 0, 3, 1, 2, 3, 1,
)


def kernel(
    u_hbm, v_hbm, ranks, model_hbm, observed_hbm, step,
    model_out, misfit_out,
    model_in, observed, u_raw, v_raw, u_tiles, v_tiles, wide, expanded_f, expanded_b,
    model_t, observed_t, misfit_t,
    x_all, sum_a, sum_b, got_a, got_b, keep_a, keep_b, next_a, next_b, last_a, last_b,
    r_a, r_b, grad, grad_got, grad_keep, grad_send, grad_last,
    load_sem, send_sem, recv_sem,
):
    freqs, rows, cols = u_raw.shape[0], u_raw.shape[1], v_tiles.shape[1]
    chains = freqs * SPLIT
    tile = v_tiles.shape[2] // 2
    half = x_all.shape[2] // 2
    col, row = lax.axis_index("col"), lax.axis_index("row")
    y, z = col // 4, col % 4
    x, core = row // 2, row % 2

    def at_y(o):
        return ((y + o) % 4 * 4 + z, row)

    def at_z(o):
        return (y * 4 + (z + o) % 4, row)

    def at_x(o):
        return (col, (x + o) % 4 * 2 + core)

    partner = (col, x * 2 + 1 - core)
    numbers = {}

    def remote(name, src, dst, device):
        number = numbers.setdefault(name, len(numbers))
        return pltpu.make_async_remote_copy(
            src_ref=src, dst_ref=dst, send_sem=send_sem.at[number], recv_sem=recv_sem.at[number],
            device_id=device, device_id_type=MESH,
        )

    side_loads = [
        pltpu.make_async_copy(src, dst, load_sem.at[2 * freqs + n])
        for n, (src, dst) in enumerate(((model_hbm, model_in), (observed_hbm, observed)))
    ]
    side_loads[0].start()
    loads = {}
    for f in range(freqs):
        for n, (src, dst) in enumerate(((v_hbm, v_raw), (u_hbm, u_raw))):
            loads[f, n] = pltpu.make_async_copy(src.at[f], dst.at[f], load_sem.at[2 * f + n])
            loads[f, n].start()

    side_loads[1].start()
    barrier = pltpu.get_barrier_semaphore()
    peers = [at_y(o) for o in (1, 2, 3)] + [at_z(o) for o in (1, 2, 3)] + [at_x(o) for o in (1, 2, 3)] + [partner]
    for peer in peers:
        pl.semaphore_signal(barrier, inc=1, device_id=peer, device_id_type=MESH)

    def chain_rows(f, turned):
        full = turned.shape[0] // 2
        return [
            (SPLIT * f + h, jnp.concatenate([turned[b + h * half:b + (h + 1) * half] for b in (0, full)], axis=0))
            for h in range(SPLIT)
        ]

    def whole_rows(f, ref):
        parts = [ref[SPLIT * f + h] for h in range(SPLIT)]
        return jnp.concatenate([part[:half] for part in parts] + [part[half:] for part in parts], axis=0).T

    side_loads[0].wait()
    for f in range(freqs):
        for c, turned in chain_rows(f, model_in[f].T):
            model_t[c] = turned
            x_all[c, row] = turned.astype(BF16)
    pl.semaphore_wait(barrier, len(peers))

    lane = lax.broadcasted_iota(jnp.int32, (1, LANES), 1)
    low = lane < LANES // 2
    lane_k = lane % (LANES // 2)

    def pick(first, second):
        return jnp.where(low, first, second)

    def swap(value):
        return pltpu.roll(value, LANES // 2, 1)

    def planes(f, raw, p):
        found = []
        for e in range(2):
            wide[e] = raw[f, 2 * p + e].astype(F32)
        for j in range(cols):
            pair = []
            for e in range(2):
                piece = wide[e, pl.ds(j, tile, stride=cols), :]
                pair.append(jnp.where(lane_k < ranks[f, j, 2 * p + e], piece, 0.0))
            found.append(pair)
        return found

    def joined(first, second):
        return pick(first, swap(second)).astype(BF16), pick(swap(first), second).astype(BF16)

    def relayout_v(f):
        loads[f, 0].wait()

        def one(p, carry):
            at = pl.ds(pl.multiple_of(p * LANES, LANES), LANES)
            for j, pair in enumerate(planes(f, v_raw, p)):
                real, imaginary = joined(pair[j % 2], pair[1 - j % 2])
                v_tiles[f, j, :tile, at] = real
                v_tiles[f, j, tile:, at] = imaginary
            return carry

        lax.fori_loop(0, rows // 2, one, 0)

    def relayout_u(f):
        loads[f, 1].wait()

        def one(p, carry):
            found = planes(f, u_raw, p)
            for e in range(2):
                for jp in range(cols // 2):
                    real, imaginary = joined(found[2 * jp + e][e], found[2 * jp + 1 - e][e])
                    u_tiles[f, 2 * p + e, :tile, jp * LANES:(jp + 1) * LANES] = real
                    u_tiles[f, 2 * p + e, tile:, jp * LANES:(jp + 1) * LANES] = imaginary
            return carry

        lax.fori_loop(0, rows // 2, one, 0)

    def gather_x_copies(f):
        own = x_all.at[f, row]
        return [remote(("a", f, o), own, own, at_x(o)) for o in (1, 3, 2)] + [remote(("a", f, 0), own, own, partner)]

    def gather_x_pass(f):
        copies = []
        for o in (1, 3, 2):
            slot = x_all.at[f, (x - o + 4) % 4 * 2 + core]
            copies.append(remote(("ap", f, o), slot, slot, partner))
        return copies

    def gather_x_start(f):
        for copy in gather_x_copies(f):
            copy.start()

    def gather_x_mid(f):
        for copy, onward in zip(gather_x_copies(f)[:3], gather_x_pass(f)):
            copy.wait_recv()
            onward.start()

    def gather_x_end(f):
        copies = gather_x_copies(f)
        copies[3].wait_recv()
        for onward in gather_x_pass(f):
            onward.wait()
        for copy in copies:
            copy.wait_send()

    def adjoint_left(value):
        return jnp.concatenate([value, jnp.concatenate([value[half:], -value[:half]], axis=0)], axis=1)

    def turned_left(value):
        return jnp.concatenate([-value[half:], value[:half]], axis=0)

    def forward_products(f):
        for jp in range(cols // 2):
            lefts = []
            for e in range(2):
                at = 2 * (2 * jp + e)
                lefts.append(adjoint_left(jnp.concatenate([x_all[f, at], x_all[f, at + 1]], axis=1)))
            for q in range(rows // 4):
                even, odd = (
                    jnp.dot(
                        lefts[e], v_tiles[f // SPLIT, 2 * jp + e, :, q * tile:(q + 1) * tile],
                        preferred_element_type=F32,
                    )
                    for e in range(2)
                )
                for p in range(2):
                    one_even, one_odd = even[:, p * LANES:(p + 1) * LANES], odd[:, p * LANES:(p + 1) * LANES]
                    i = 4 * q + 2 * p
                    expanded_f[i, :, jp * LANES:(jp + 1) * LANES] = pick(one_even, one_odd).astype(BF16)
                    expanded_f[i + 1, :, jp * LANES:(jp + 1) * LANES] = pick(one_odd, one_even).astype(BF16)

    def forward_sums(f):
        for i in range(rows):
            left = expanded_f[i]
            total = lax.dot_general(left, u_tiles[f // SPLIT, i, :tile], TRANS_B, preferred_element_type=F32)
            total = total + lax.dot_general(
                turned_left(left), u_tiles[f // SPLIT, i, tile:], TRANS_B, preferred_element_type=F32
            )
            total = total.astype(BF16)
            for h in range(2):
                part = total[:, h * LANES:(h + 1) * LANES]
                sum_a[f, 2 * i + h] = part[:half]
                sum_b[f, (2 * (i % 2) + h) * 4 + i // 2] = part[half:]

    def first_copies(f):
        copies = []
        for o in (1, 3, 2):
            copies.append(remote(("c1a", f, o), sum_a.at[f, pl.ds((y + o) % 4 * 4, 4)], got_a.at[f, o - 1], at_y(o)))
            copies.append(remote(("c1b", f, o), sum_b.at[f, pl.ds((z + o) % 4 * 4, 4)], got_b.at[f, o - 1], at_z(o)))
        return copies

    def second_copies(f):
        copies = []
        for o in (1, 3, 2):
            copies.append(remote(("c2a", f, o), next_a.at[f, (z + o) % 4], last_a.at[f, o - 1], at_z(o)))
            copies.append(remote(("c2b", f, o), next_b.at[f, (y + o) % 4], last_b.at[f, o - 1], at_y(o)))
        return copies

    def start(copies):
        for copy in copies:
            copy.start()

    def wait(copies):
        for copy in copies:
            copy.wait()

    def first_end(f):
        wait(first_copies(f))
        for q in range(4):
            for own, got, keep, onward, at in (
                (sum_a, got_a, keep_a, next_a, y), (sum_b, got_b, keep_b, next_b, z)
            ):
                total = own[f, at * 4 + q].astype(F32)
                for o in range(3):
                    total = total + got[f, o, q].astype(F32)
                keep[f, q] = total
                onward[f, q] = total.astype(BF16)
        start(second_copies(f))

    def gather_first(f):
        copies = []
        own_a, own_b = r_a.at[f, y * 4 + z], r_b.at[f, z * 4 + y]
        for o in (1, 3, 2):
            copies.append(remote(("e1a", f, o), own_a, own_a, at_z(o)))
            copies.append(remote(("e1b", f, o), own_b, own_b, at_y(o)))
        return copies

    def gather_second(f):
        copies = []
        own_a, own_b = r_a.at[f, pl.ds(y * 4, 4)], r_b.at[f, pl.ds(z * 4, 4)]
        for o in (1, 3, 2):
            copies.append(remote(("e2a", f, o), own_a, own_a, at_y(o)))
            copies.append(remote(("e2b", f, o), own_b, own_b, at_z(o)))
        return copies

    def second_end(f, last):
        wait(second_copies(f))
        for keep, got, to, rows_at, at, slot in (
            (keep_a, last_a, r_a, slice(0, half), z, y * 4 + z),
            (keep_b, last_b, r_b, slice(half, tile), y, z * 4 + y),
        ):
            total = keep[f, at]
            for o in range(3):
                total = total + got[f, o].astype(F32)
            total = total - observed_t[f, rows_at]
            if last:
                misfit_t[f, rows_at] = total
            to[f, slot] = total.astype(BF16)
        start(gather_first(f))

    def backward_products(f):
        for p in range(rows // 2):
            found = []
            for e in range(2):
                i = 2 * p + e
                left_a = jnp.concatenate([r_a[f, 2 * i], r_a[f, 2 * i + 1]], axis=1)
                left_b = jnp.concatenate([r_b[f, 8 * e + p], r_b[f, 8 * e + 4 + p]], axis=1)
                left = adjoint_left(jnp.concatenate([left_a, left_b], axis=0))
                found.append(jnp.dot(left, u_tiles[f // SPLIT, i], preferred_element_type=F32))
            for jp in range(cols // 2):
                even, odd = (value[:, jp * LANES:(jp + 1) * LANES] for value in found)
                expanded_b[2 * jp, :, p * LANES:(p + 1) * LANES] = pick(even, odd).astype(BF16)
                expanded_b[2 * jp + 1, :, p * LANES:(p + 1) * LANES] = pick(odd, even).astype(BF16)

    def pair_copy(f, j):
        return remote(("g1", f, j), grad.at[f, 1 - core, j], grad_got.at[f, j], partner)

    def backward_sums(f):
        for j in range(cols):
            left = expanded_b[j]
            total = lax.dot_general(left, v_tiles[f // SPLIT, j, :tile], TRANS_B, preferred_element_type=F32)
            total = total + lax.dot_general(
                turned_left(left), v_tiles[f // SPLIT, j, tile:], TRANS_B, preferred_element_type=F32
            )
            for h in range(2):
                grad[f, h, j] = total[:, h * LANES:(h + 1) * LANES]
            pair_copy(f, j).start()

    def across_copies(f):
        return [
            remote(("g2", f, o), grad_send.at[f, (x + o) % 4], grad_last.at[f, o - 1], at_x(o)) for o in (1, 3, 2)
        ]

    def pair_end(f):
        for j in range(cols):
            pair_copy(f, j).wait()
            total = grad[f, core, j] + grad_got[f, j]
            grad_keep[f, j] = total
            grad_send[f, j] = total.astype(BF16)
        start(across_copies(f))

    def across_end(f, last):
        wait(across_copies(f))
        total = grad_keep[f, x]
        for o in range(3):
            total = total + grad_last[f, o].astype(F32)
        new = model_t[f] - step[f // SPLIT] * total
        model_t[f] = new
        if not last:
            x_all[f, row] = new.astype(BF16)
            gather_x_start(f)

    def prepare(f):
        relayout_v(f)
        relayout_u(f)
        if f == 0:
            side_loads[1].wait()
        for c, turned in chain_rows(f, observed[f].T):
            observed_t[c] = turned

    def stages(f):
        gather_x_start(f)
        if f == chains - 1:
            prepare(0)
        yield
        for sweep in range(ITERS):
            last = sweep == ITERS - 1
            gather_x_mid(f)
            yield
            if sweep == 0 and f % SPLIT == 0 and f > 0:
                prepare(f // SPLIT)
            gather_x_end(f)
            forward_products(f)
            forward_sums(f)
            start(first_copies(f))
            yield
            first_end(f)
            yield
            second_end(f, last)
            yield
            wait(gather_first(f))
            start(gather_second(f))
            if last and f % SPLIT == SPLIT - 1:
                misfit_out[f // SPLIT] = whole_rows(f // SPLIT, misfit_t)
            yield
            wait(gather_second(f))
            backward_products(f)
            backward_sums(f)
            yield
            pair_end(f)
            yield
            across_end(f, last)
            if last and f % SPLIT == SPLIT - 1:
                model_out[f // SPLIT] = whole_rows(f // SPLIT, model_t)
            yield

    running = [stages(f) for f in range(chains)]
    for f in ORDER:
        next(running[f])


def local(u_factors, v_factors, ranks, model_init, observed, step):
    freqs, rows, tile, cols, width = u_factors.shape
    both, share = model_init.shape[2], model_init.shape[1]
    chains, part = freqs * SPLIT, both // SPLIT
    half = part // 2
    raw = (freqs, rows, tile * cols, width)
    vmem = lambda shape, kind: pltpu.VMEM(shape, kind)
    scratch = [
        vmem(model_init.shape, F32), vmem(observed.shape, F32), vmem(raw, BF16), vmem(raw, BF16),
        vmem((freqs, rows, 2 * tile, cols * width // 2), BF16), vmem((freqs, cols, 2 * tile, rows * width // 2), BF16),
        vmem((2, tile * cols, width), F32),
        vmem((rows, part, cols * width // 2), BF16), vmem((cols, part, rows * width // 2), BF16),
        vmem((chains, part, share), F32), vmem((chains, part, share), F32), vmem((chains, part, share), F32),
        vmem((chains, 8, part, share), BF16),
        vmem((chains, 16, half, share), BF16), vmem((chains, 16, half, share), BF16),
        vmem((chains, 3, 4, half, share), BF16), vmem((chains, 3, 4, half, share), BF16),
        vmem((chains, 4, half, share), F32), vmem((chains, 4, half, share), F32),
        vmem((chains, 4, half, share), BF16), vmem((chains, 4, half, share), BF16),
        vmem((chains, 3, half, share), BF16), vmem((chains, 3, half, share), BF16),
        vmem((chains, 16, half, share), BF16), vmem((chains, 16, half, share), BF16),
        vmem((chains, 2, cols, part, share), F32), vmem((chains, cols, part, share), F32),
        vmem((chains, cols, part, share), F32), vmem((chains, cols, part, share), BF16),
        vmem((chains, 3, part, share), BF16),
        pltpu.SemaphoreType.DMA((2 * freqs + 2,)),
        pltpu.SemaphoreType.DMA((38 * chains,)), pltpu.SemaphoreType.DMA((38 * chains,)),
    ]
    in_vmem = pl.BlockSpec(memory_space=pltpu.VMEM)
    in_smem = pl.BlockSpec(memory_space=pltpu.SMEM)
    anywhere = pl.BlockSpec(memory_space=pl.ANY)
    return pl.pallas_call(
        kernel,
        out_shape=(
            jax.ShapeDtypeStruct(model_init.shape, F32), jax.ShapeDtypeStruct(observed.shape, F32),
        ),
        in_specs=[anywhere, anywhere, in_smem, anywhere, anywhere, in_smem],
        out_specs=(in_vmem, in_vmem),
        scratch_shapes=scratch,
        compiler_params=pltpu.CompilerParams(
            collective_id=0, has_side_effects=True, vmem_limit_bytes=int(53.25 * 2**20)
        ),
    )(u_factors.reshape(raw), v_factors.reshape(raw), ranks.transpose(0, 2, 1), model_init, observed, step)


def solution(mesh):
    return jax.shard_map(
        local,
        mesh=mesh,
        in_specs=(
            P(None, "row", None, "col", None),
            P(None, "row", None, "col", None),
            P(None, "row", "col"),
            P(None, ("col", "row"), None),
            P(None, ("row", "col"), None),
            P(),
        ),
        out_specs=(P(None, ("col", "row"), None), P(None, ("row", "col"), None)),
        check_vma=False,
    )
```

```python
import functools

import jax
import jax.numpy as jnp
from jax import lax
from jax.experimental import pallas as pl
from jax.experimental.pallas import tpu as pltpu
from jax.sharding import PartitionSpec as P

ITERS = 2
MESH = pl.DeviceIdType.MESH
F32, BF16 = jnp.float32, jnp.bfloat16
LANES = 128
TRANS_B = (((1,), (1,)), ((), ()))
SPLIT = 2
ORDER = (
    0, 1, 2, 3, 0, 0, 2, 2, 3, 1, 0, 3, 2, 0, 1, 2, 3,
    0, 1, 3, 2, 0, 1, 3, 0, 2, 1, 2, 0, 3, 3, 1, 2, 0,
    1, 0, 3, 2, 2, 1, 3, 0, 3, 1, 2, 0, 1, 3, 2, 0, 1,
    3, 2, 1, 3, 0, 1, 2, 0, 3, 2, 1, 0, 3, 1, 2, 3, 1,
)


def kernel(
    u_hbm, v_hbm, ranks, model_hbm, observed_hbm, step,
    model_out, misfit_out,
    model_in, observed, u_raw, v_raw, u_tiles, v_tiles, wide, expanded_f, expanded_b,
    model_t, observed_t, misfit_t,
    x_all, sum_a, sum_b, got_a, got_b, keep_a, keep_b, next_a, next_b, last_a, last_b,
    r_a, r_b, grad, grad_got, grad_keep, grad_send, grad_last,
    load_sem, send_sem, recv_sem,
):
    freqs, rows, cols = u_raw.shape[0], u_raw.shape[1], v_tiles.shape[1]
    chains = freqs * SPLIT
    tile = v_tiles.shape[2] // 2
    half = x_all.shape[2] // 2
    col, row = lax.axis_index("col"), lax.axis_index("row")
    y, z = col // 4, col % 4
    x, core = row // 2, row % 2

    def at_y(o):
        return ((y + o) % 4 * 4 + z, row)

    def at_z(o):
        return (y * 4 + (z + o) % 4, row)

    def at_x(o):
        return (col, (x + o) % 4 * 2 + core)

    partner = (col, x * 2 + 1 - core)
    numbers = {}

    def remote(name, src, dst, device):
        number = numbers.setdefault(name, len(numbers))
        return pltpu.make_async_remote_copy(
            src_ref=src, dst_ref=dst, send_sem=send_sem.at[number], recv_sem=recv_sem.at[number],
            device_id=device, device_id_type=MESH,
        )

    side_loads = [
        pltpu.make_async_copy(src, dst, load_sem.at[2 * freqs + n])
        for n, (src, dst) in enumerate(((model_hbm, model_in), (observed_hbm, observed)))
    ]
    side_loads[0].start()
    loads = {}
    for f in range(freqs):
        for n, (src, dst) in enumerate(((v_hbm, v_raw), (u_hbm, u_raw))):
            loads[f, n] = pltpu.make_async_copy(src.at[f], dst.at[f], load_sem.at[2 * f + n])
            loads[f, n].start()

    side_loads[1].start()
    barrier = pltpu.get_barrier_semaphore()
    peers = [at_y(o) for o in (1, 2, 3)] + [at_z(o) for o in (1, 2, 3)] + [at_x(o) for o in (1, 2, 3)] + [partner]
    for peer in peers:
        pl.semaphore_signal(barrier, inc=1, device_id=peer, device_id_type=MESH)

    def chain_rows(f, turned):
        full = turned.shape[0] // 2
        return [
            (SPLIT * f + h, jnp.concatenate([turned[b + h * half:b + (h + 1) * half] for b in (0, full)], axis=0))
            for h in range(SPLIT)
        ]

    def whole_rows(f, ref):
        parts = [ref[SPLIT * f + h] for h in range(SPLIT)]
        return jnp.concatenate([part[:half] for part in parts] + [part[half:] for part in parts], axis=0).T

    side_loads[0].wait()
    for f in range(freqs):
        for c, turned in chain_rows(f, model_in[f].T):
            model_t[c] = turned
            x_all[c, row] = turned.astype(BF16)
    pl.semaphore_wait(barrier, len(peers))

    lane = lax.broadcasted_iota(jnp.int32, (1, LANES), 1)
    low = lane < LANES // 2
    lane_k = lane % (LANES // 2)

    def pick(first, second):
        return jnp.where(low, first, second)

    def swap(value):
        return pltpu.roll(value, LANES // 2, 1)

    def planes(f, raw, p):
        found = []
        for e in range(2):
            wide[e] = raw[f, 2 * p + e].astype(F32)
        for j in range(cols):
            pair = []
            for e in range(2):
                piece = wide[e, pl.ds(j, tile, stride=cols), :]
                pair.append(jnp.where(lane_k < ranks[f, j, 2 * p + e], piece, 0.0))
            found.append(pair)
        return found

    def joined(first, second):
        return pick(first, swap(second)).astype(BF16), pick(swap(first), second).astype(BF16)

    def relayout_v(f):
        loads[f, 0].wait()

        def one(p, carry):
            at = pl.ds(pl.multiple_of(p * LANES, LANES), LANES)
            for j, pair in enumerate(planes(f, v_raw, p)):
                real, imaginary = joined(pair[j % 2], pair[1 - j % 2])
                v_tiles[f, j, :tile, at] = real
                v_tiles[f, j, tile:, at] = imaginary
            return carry

        lax.fori_loop(0, rows // 2, one, 0)

    def relayout_u(f):
        loads[f, 1].wait()

        def one(p, carry):
            found = planes(f, u_raw, p)
            for e in range(2):
                for jp in range(cols // 2):
                    real, imaginary = joined(found[2 * jp + e][e], found[2 * jp + 1 - e][e])
                    u_tiles[f, 2 * p + e, :tile, jp * LANES:(jp + 1) * LANES] = real
                    u_tiles[f, 2 * p + e, tile:, jp * LANES:(jp + 1) * LANES] = imaginary
            return carry

        lax.fori_loop(0, rows // 2, one, 0)

    def gather_x_copies(f):
        own = x_all.at[f, row]
        return [remote(("a", f, o), own, own, at_x(o)) for o in (1, 3, 2)] + [remote(("a", f, 0), own, own, partner)]

    def gather_x_pass(f):
        copies = []
        for o in (1, 3, 2):
            slot = x_all.at[f, (x - o + 4) % 4 * 2 + core]
            copies.append(remote(("ap", f, o), slot, slot, partner))
        return copies

    def gather_x_start(f):
        for copy in gather_x_copies(f):
            copy.start()

    def gather_x_mid(f):
        for copy, onward in zip(gather_x_copies(f)[:3], gather_x_pass(f)):
            copy.wait_recv()
            onward.start()

    def gather_x_end(f):
        copies = gather_x_copies(f)
        copies[3].wait_recv()
        for onward in gather_x_pass(f):
            onward.wait()
        for copy in copies:
            copy.wait_send()

    def adjoint_left(value):
        return jnp.concatenate([value, jnp.concatenate([value[half:], -value[:half]], axis=0)], axis=1)

    def turned_left(value):
        return jnp.concatenate([-value[half:], value[:half]], axis=0)

    def forward_products(f):
        for jp in range(cols // 2):
            lefts = []
            for e in range(2):
                at = 2 * (2 * jp + e)
                lefts.append(adjoint_left(jnp.concatenate([x_all[f, at], x_all[f, at + 1]], axis=1)))
            for q in range(rows // 4):
                even, odd = (
                    jnp.dot(
                        lefts[e], v_tiles[f // SPLIT, 2 * jp + e, :, q * tile:(q + 1) * tile],
                        preferred_element_type=F32,
                    )
                    for e in range(2)
                )
                for p in range(2):
                    one_even, one_odd = even[:, p * LANES:(p + 1) * LANES], odd[:, p * LANES:(p + 1) * LANES]
                    i = 4 * q + 2 * p
                    expanded_f[i, :, jp * LANES:(jp + 1) * LANES] = pick(one_even, one_odd).astype(BF16)
                    expanded_f[i + 1, :, jp * LANES:(jp + 1) * LANES] = pick(one_odd, one_even).astype(BF16)

    def forward_sums(f):
        for i in range(rows):
            left = expanded_f[i]
            total = lax.dot_general(left, u_tiles[f // SPLIT, i, :tile], TRANS_B, preferred_element_type=F32)
            total = total + lax.dot_general(
                turned_left(left), u_tiles[f // SPLIT, i, tile:], TRANS_B, preferred_element_type=F32
            )
            total = total.astype(BF16)
            for h in range(2):
                part = total[:, h * LANES:(h + 1) * LANES]
                sum_a[f, 2 * i + h] = part[:half]
                sum_b[f, (2 * (i % 2) + h) * 4 + i // 2] = part[half:]

    def first_copies(f):
        copies = []
        for o in (1, 3, 2):
            copies.append(remote(("c1a", f, o), sum_a.at[f, pl.ds((y + o) % 4 * 4, 4)], got_a.at[f, o - 1], at_y(o)))
            copies.append(remote(("c1b", f, o), sum_b.at[f, pl.ds((z + o) % 4 * 4, 4)], got_b.at[f, o - 1], at_z(o)))
        return copies

    def second_copies(f):
        copies = []
        for o in (1, 3, 2):
            copies.append(remote(("c2a", f, o), next_a.at[f, (z + o) % 4], last_a.at[f, o - 1], at_z(o)))
            copies.append(remote(("c2b", f, o), next_b.at[f, (y + o) % 4], last_b.at[f, o - 1], at_y(o)))
        return copies

    def start(copies):
        for copy in copies:
            copy.start()

    def wait(copies):
        for copy in copies:
            copy.wait()

    def first_end(f):
        arriving, leaving = first_copies(f), second_copies(f)
        for n, (own, got, keep, onward, at) in enumerate((
            (sum_a, got_a, keep_a, next_a, y), (sum_b, got_b, keep_b, next_b, z)
        )):
            wait(arriving[n::2])
            for q in range(4):
                total = own[f, at * 4 + q].astype(F32)
                for o in range(3):
                    total = total + got[f, o, q].astype(F32)
                keep[f, q] = total
                onward[f, q] = total.astype(BF16)
            start(leaving[n::2])

    def gather_first(f):
        copies = []
        own_a, own_b = r_a.at[f, y * 4 + z], r_b.at[f, z * 4 + y]
        for o in (1, 3, 2):
            copies.append(remote(("e1a", f, o), own_a, own_a, at_z(o)))
            copies.append(remote(("e1b", f, o), own_b, own_b, at_y(o)))
        return copies

    def gather_second(f):
        copies = []
        own_a, own_b = r_a.at[f, pl.ds(y * 4, 4)], r_b.at[f, pl.ds(z * 4, 4)]
        for o in (1, 3, 2):
            copies.append(remote(("e2a", f, o), own_a, own_a, at_y(o)))
            copies.append(remote(("e2b", f, o), own_b, own_b, at_z(o)))
        return copies

    def second_end(f, last):
        arriving, leaving = second_copies(f), gather_first(f)
        for n, (keep, got, to, rows_at, at, slot) in enumerate((
            (keep_a, last_a, r_a, slice(0, half), z, y * 4 + z),
            (keep_b, last_b, r_b, slice(half, 2 * half), y, z * 4 + y),
        )):
            wait(arriving[n::2])
            total = keep[f, at]
            for o in range(3):
                total = total + got[f, o].astype(F32)
            total = total - observed_t[f, rows_at]
            if last:
                misfit_t[f, rows_at] = total
            to[f, slot] = total.astype(BF16)
            start(leaving[n::2])

    def backward_products(f):
        for p in range(rows // 2):
            found = []
            for e in range(2):
                i = 2 * p + e
                left_a = jnp.concatenate([r_a[f, 2 * i], r_a[f, 2 * i + 1]], axis=1)
                left_b = jnp.concatenate([r_b[f, 8 * e + p], r_b[f, 8 * e + 4 + p]], axis=1)
                left = adjoint_left(jnp.concatenate([left_a, left_b], axis=0))
                found.append(jnp.dot(left, u_tiles[f // SPLIT, i], preferred_element_type=F32))
            for jp in range(cols // 2):
                even, odd = (value[:, jp * LANES:(jp + 1) * LANES] for value in found)
                expanded_b[2 * jp, :, p * LANES:(p + 1) * LANES] = pick(even, odd).astype(BF16)
                expanded_b[2 * jp + 1, :, p * LANES:(p + 1) * LANES] = pick(odd, even).astype(BF16)

    def pair_copy(f, j):
        return remote(("g1", f, j), grad.at[f, 1 - core, j], grad_got.at[f, j], partner)

    def backward_sums(f):
        for j in range(cols):
            left = expanded_b[j]
            total = lax.dot_general(left, v_tiles[f // SPLIT, j, :tile], TRANS_B, preferred_element_type=F32)
            total = total + lax.dot_general(
                turned_left(left), v_tiles[f // SPLIT, j, tile:], TRANS_B, preferred_element_type=F32
            )
            for h in range(2):
                grad[f, h, j] = total[:, h * LANES:(h + 1) * LANES]
            pair_copy(f, j).start()

    def across_copies(f):
        return [
            remote(("g2", f, o), grad_send.at[f, (x + o) % 4], grad_last.at[f, o - 1], at_x(o)) for o in (1, 3, 2)
        ]

    def pair_end(f):
        for j in range(cols):
            pair_copy(f, j).wait()
            total = grad[f, core, j] + grad_got[f, j]
            grad_keep[f, j] = total
            grad_send[f, j] = total.astype(BF16)
        start(across_copies(f))

    def across_end(f, last):
        wait(across_copies(f))
        total = grad_keep[f, x]
        for o in range(3):
            total = total + grad_last[f, o].astype(F32)
        new = model_t[f] - step[f // SPLIT] * total
        model_t[f] = new
        if not last:
            x_all[f, row] = new.astype(BF16)
            gather_x_start(f)

    def prepare(f):
        relayout_v(f)
        relayout_u(f)
        if f == 0:
            side_loads[1].wait()
        for c, turned in chain_rows(f, observed[f].T):
            observed_t[c] = turned

    def stages(f):
        gather_x_start(f)
        if f == chains - 1:
            prepare(0)
        yield
        for sweep in range(ITERS):
            last = sweep == ITERS - 1
            gather_x_mid(f)
            yield
            if sweep == 0 and f % SPLIT == 0 and f > 0:
                prepare(f // SPLIT)
            gather_x_end(f)
            forward_products(f)
            forward_sums(f)
            start(first_copies(f))
            yield
            first_end(f)
            yield
            second_end(f, last)
            yield
            wait(gather_first(f))
            start(gather_second(f))
            if last and f % SPLIT == SPLIT - 1:
                misfit_out[f // SPLIT] = whole_rows(f // SPLIT, misfit_t)
            yield
            wait(gather_second(f))
            backward_products(f)
            backward_sums(f)
            yield
            pair_end(f)
            yield
            across_end(f, last)
            if last and f % SPLIT == SPLIT - 1:
                model_out[f // SPLIT] = whole_rows(f // SPLIT, model_t)
            yield

    running = [stages(f) for f in range(chains)]
    for f in ORDER:
        next(running[f])


def local(u_factors, v_factors, ranks, model_init, observed, step):
    freqs, rows, tile, cols, width = u_factors.shape
    both, share = model_init.shape[2], model_init.shape[1]
    chains, part = freqs * SPLIT, both // SPLIT
    half = part // 2
    raw = (freqs, rows, tile * cols, width)
    vmem = lambda shape, kind: pltpu.VMEM(shape, kind)
    scratch = [
        vmem(model_init.shape, F32), vmem(observed.shape, F32), vmem(raw, BF16), vmem(raw, BF16),
        vmem((freqs, rows, 2 * tile, cols * width // 2), BF16), vmem((freqs, cols, 2 * tile, rows * width // 2), BF16),
        vmem((2, tile * cols, width), F32),
        vmem((rows, part, cols * width // 2), BF16), vmem((cols, part, rows * width // 2), BF16),
        vmem((chains, part, share), F32), vmem((chains, part, share), F32), vmem((chains, part, share), F32),
        vmem((chains, 8, part, share), BF16),
        vmem((chains, 16, half, share), BF16), vmem((chains, 16, half, share), BF16),
        vmem((chains, 3, 4, half, share), BF16), vmem((chains, 3, 4, half, share), BF16),
        vmem((chains, 4, half, share), F32), vmem((chains, 4, half, share), F32),
        vmem((chains, 4, half, share), BF16), vmem((chains, 4, half, share), BF16),
        vmem((chains, 3, half, share), BF16), vmem((chains, 3, half, share), BF16),
        vmem((chains, 16, half, share), BF16), vmem((chains, 16, half, share), BF16),
        vmem((chains, 2, cols, part, share), F32), vmem((chains, cols, part, share), F32),
        vmem((chains, cols, part, share), F32), vmem((chains, cols, part, share), BF16),
        vmem((chains, 3, part, share), BF16),
        pltpu.SemaphoreType.DMA((2 * freqs + 2,)),
        pltpu.SemaphoreType.DMA((38 * chains,)), pltpu.SemaphoreType.DMA((38 * chains,)),
    ]
    in_vmem = pl.BlockSpec(memory_space=pltpu.VMEM)
    in_smem = pl.BlockSpec(memory_space=pltpu.SMEM)
    anywhere = pl.BlockSpec(memory_space=pl.ANY)
    return pl.pallas_call(
        kernel,
        out_shape=(
            jax.ShapeDtypeStruct(model_init.shape, F32), jax.ShapeDtypeStruct(observed.shape, F32),
        ),
        in_specs=[anywhere, anywhere, in_smem, anywhere, anywhere, in_smem],
        out_specs=(in_vmem, in_vmem),
        scratch_shapes=scratch,
        compiler_params=pltpu.CompilerParams(
            collective_id=0, has_side_effects=True, vmem_limit_bytes=int(53.25 * 2**20)
        ),
    )(u_factors.reshape(raw), v_factors.reshape(raw), ranks.transpose(0, 2, 1), model_init, observed, step)


def solution(mesh):
    return jax.shard_map(
        local,
        mesh=mesh,
        in_specs=(
            P(None, "row", None, "col", None),
            P(None, "row", None, "col", None),
            P(None, "row", "col"),
            P(None, ("col", "row"), None),
            P(None, ("row", "col"), None),
            P(),
        ),
        out_specs=(P(None, ("col", "row"), None), P(None, ("row", "col"), None)),
        check_vma=False,
    )
```
